8 devices in a mesh: dp: 2 (over y, z), tp: 4 (over x, core).
Axes of the slice: x: 2, y: 2, z: 1, core: 2. Of those that a mesh axis runs over, the one named last changes fastest.
Arguments:
- x: bfloat16 [4096, 2048], P(('dp', 'tp')), parts along dimension 0
- gain: bfloat16 [2048], replicated
- wq: bfloat16 [2048, 4096], P(None, 'tp')
- wk: bfloat16 [2048, 2048], P(None, 'tp')
- wv: bfloat16 [2048, 2048], P(None, 'tp')
- wo: bfloat16 [4096, 2048], P('tp')
Outputs:
- output: bfloat16 [4096, 2048], P(('dp', 'tp')), parts along dimension 0
There are 2 independent parts. The reference program is written for one: setup_inputs(seed, part) draws one part's arguments, and reference() takes and returns one part's arrays. A program takes and returns all parts, laid end to end along the dimension named above; an argument that names none is the same for every part.
All inputs are finite; a program needn't handle non-finite values.
Results may differ from the reference program's by a relative error of at most 0.012.
Values are sent between devices in bfloat16 or wider.
A program may use at most 2 GiB of HBM per device.

```python
import jax
import jax.numpy as jnp
from jax import lax

ROWS = 2048
D = 2048
HEADS = 32
KV_HEADS = 16
HEAD = 128
THETA = 10000


def setup_inputs(seed: int = 0, part: int = 0) -> dict:
    kx, kn, kq, kk, kv, ko = jax.random.split(jax.random.key(seed), 6)

    def weights(key, rows, columns):
        return jax.random.normal(key, (rows, columns), jnp.float32) * rows**-0.5

    drawn = {
        "x": jax.random.normal(jax.random.fold_in(kx, part), (ROWS, D), jnp.float32),
        "gain": 1 + 0.1 * jax.random.normal(kn, (D,), jnp.float32),
        "wq": 2 * weights(kq, D, HEADS * HEAD),
        "wk": 2 * weights(kk, D, KV_HEADS * HEAD),
        "wv": 4 * weights(kv, D, KV_HEADS * HEAD),
        "wo": weights(ko, HEADS * HEAD, D),
    }
    return {k: v.astype(jnp.bfloat16) for k, v in drawn.items()}


def normed(x, gain):
    wide = x.astype(jnp.float32)
    scale = lax.rsqrt(jnp.mean(wide * wide, -1, keepdims=True) + 1e-6)
    return (wide * scale * gain.astype(jnp.float32)).astype(jnp.bfloat16)


def turned(t, place, theta):
    half = t.shape[-1] // 2
    angle = place.astype(jnp.float32)[:, None] * theta ** (-jnp.arange(half, dtype=jnp.float32) / half)
    cos, sin = jnp.cos(angle)[:, None], jnp.sin(angle)[:, None]
    a, b = t[..., :half].astype(jnp.float32), t[..., half:].astype(jnp.float32)
    return jnp.concatenate([a * cos - b * sin, b * cos + a * sin], -1).astype(jnp.bfloat16)


def matmul(a, w):
    return jnp.dot(a, w, preferred_element_type=jnp.float32).astype(jnp.bfloat16)


def einsum(form, a, b):
    return jnp.einsum(form, a.astype(jnp.float32), b.astype(jnp.float32))


def attention(q, k, v):
    scores = einsum("tgsd,ugd->gstu", q, k) * q.shape[-1] ** -0.5
    token = jnp.arange(q.shape[0])
    scores = jnp.where(token[:, None] >= token, scores, -jnp.inf)
    weights = jax.nn.softmax(scores, -1).astype(jnp.bfloat16)
    return einsum("gstu,ugd->tgsd", weights, v).astype(jnp.bfloat16)


def reference(x, gain, wq, wk, wv, wo):
    a, place = normed(x, gain), jnp.arange(ROWS)
    q = turned(matmul(a, wq).reshape(ROWS, HEADS, HEAD), place, THETA).reshape(ROWS, KV_HEADS, -1, HEAD)
    k = turned(matmul(a, wk).reshape(ROWS, KV_HEADS, HEAD), place, THETA)
    v = matmul(a, wv).reshape(ROWS, KV_HEADS, HEAD)
    seen = attention(q, k, v).reshape(ROWS, HEADS * HEAD)
    return (x.astype(jnp.float32) + jnp.dot(seen, wo, preferred_element_type=jnp.float32)).astype(jnp.bfloat16)
```

```python
import functools

import jax
import jax.numpy as jnp
import numpy as np
from jax import lax
from jax.experimental import pallas as pl
from jax.experimental.pallas import tpu as pltpu
from jax.sharding import PartitionSpec as P

HEAD = 128
THETA = 10000
NEG = -1e30
HIDDEN = 2 * NEG
SCALE2 = HEAD**-0.5 * 1.4426950408889634
ROWS, WIDE = 2048, 2048
PAIR, CHUNK = 256, 128
KV = 4
COLS = 2 * PAIR
VMEM = 67043328
MESH = pl.DeviceIdType.MESH
bf16, f32 = jnp.bfloat16, jnp.float32


def _dot(a, b, ca, cb):
    return lax.dot_general(a, b, (((ca,), (cb,)), ((), ())), preferred_element_type=f32)


def _turned(t, cos, sin):
    wide = t.astype(bf16).astype(f32)
    return (wide * cos + pltpu.roll(wide, HEAD // 2, 1) * sin).astype(bf16)


def _project(xs, wq, wk, wv, cos, sin, q_dst, k_s, v_s, at):
    here = pl.ds(at, PAIR)
    for n in range(KV // 2):
        r = jnp.dot(xs[...], wk[:, n * 256 : (n + 1) * 256], preferred_element_type=f32)
        for i in range(2):
            k_s[2 * n + i, here, :] = _turned(r[:, i * HEAD : (i + 1) * HEAD], cos[...], sin[...])
    for n in range(KV // 2):
        r = jnp.dot(xs[...], wv[:, n * 256 : (n + 1) * 256], preferred_element_type=f32).astype(bf16)
        for i in range(2):
            v_s[2 * n + i, :HEAD, here] = r[:, i * HEAD : (i + 1) * HEAD].T
    for n in range(KV):
        r = jnp.dot(xs[...], wq[:, n * 256 : (n + 1) * 256], preferred_element_type=f32)
        for i in range(2):
            q_dst[n, i * PAIR : (i + 1) * PAIR, :] = _turned(r[:, i * HEAD : (i + 1) * HEAD], cos[...], sin[...])


def _block(q, k_s, v_s, top_s, mix_s, at, size, ok=None):
    here = pl.ds(at, size)
    scores = [_dot(k_s[i, here, :], q[i], 1, 1) for i in range(KV)]
    weights, keeps = [], []
    for i, s in enumerate(scores):
        if ok is not None:
            s = jnp.where(ok, s, HIDDEN)
        old = top_s[i : i + 1, :]
        top = jnp.maximum(old, s.max(axis=0, keepdims=True))
        top_s[i : i + 1, :] = top
        weights.append(jnp.exp2((s - top) * SCALE2).astype(bf16))
        keeps.append(jnp.exp2((old - top) * SCALE2))
    for i, (w, keep) in enumerate(zip(weights, keeps)):
        mix_s[i] = mix_s[i] * keep + _dot(v_s[i, :, here], w, 1, 0)


def _finish(mix_s, seen_s):
    for i in range(KV):
        o = (mix_s[i, :HEAD, :] * (1 / mix_s[i, HEAD : HEAD + 1, :])).astype(bf16).T
        for n in range(2):
            seen_s[:, (2 * i + n) * HEAD : (2 * i + n + 1) * HEAD] = o[n * PAIR : (n + 1) * PAIR, :]


def _kernel(x, gain, wq, wk, wv, wo, base_cos, base_sin, step_cos, step_sin, y,
            x_s, gain_s, wq_s, wk_s, wv_s, wo_s, bc_s, bs_s, sc_s, ss_s, cos_s, sin_s,
            xn_s, q_s, k_s, v_s, top_s, mix_s, gap_s, seen_s,
            hold_s, term_out, term_in, sum_out, sum_in, own_s, own_out, own_in,
            load_sem, w_sem, near_send, near_recv, link_send, link_recv, fwd_send, fwd_recv,
            term_send, term_recv, sum_send, sum_recv, own_send, own_recv, y_sem):
    me = lax.axis_index("tp")
    p, c = me // 2, me % 2
    partner, across = 2 * p + 1 - c, 2 * (1 - p) + c
    mine, theirs = 1024 * p, 1024 * (1 - p)
    start = mine + 512 * c

    def remote(src, dst, send, recv, to):
        return pltpu.make_async_remote_copy(src_ref=src, dst_ref=dst, send_sem=send, recv_sem=recv, device_id={"tp": to}, device_id_type=MESH)

    def rows(at, n):
        return xn_s.at[pl.ds(pl.multiple_of(at, CHUNK), n), :]

    def near(k):
        return remote(rows(start + PAIR * k, PAIR), rows(start + PAIR * k, PAIR), near_send.at[k], near_recv.at[k], partner)

    def near_in(k):
        at = mine + 512 * (1 - c) + PAIR * k
        return remote(rows(at, PAIR), rows(at, PAIR), near_send.at[k], near_recv.at[k], partner)

    def link(j):
        at = mine + PAIR * j + CHUNK * c
        return remote(rows(at, CHUNK), rows(at, CHUNK), link_send.at[j], link_recv.at[j], across)

    def link_in(j):
        at = theirs + PAIR * j + CHUNK * c
        return remote(rows(at, CHUNK), rows(at, CHUNK), link_send.at[j], link_recv.at[j], across)

    def forward(j):
        at = theirs + PAIR * j + CHUNK * c
        return remote(rows(at, CHUNK), rows(at, CHUNK), fwd_send.at[j], fwd_recv.at[j], partner)

    def forward_in(j):
        at = theirs + PAIR * j + CHUNK * (1 - c)
        return remote(rows(at, CHUNK), rows(at, CHUNK), fwd_send.at[j], fwd_recv.at[j], partner)

    def term(j):
        return remote(term_out.at[j], term_in.at[j], term_send.at[j], term_recv.at[j], partner)

    def total(j):
        m = (2 * j + c) % 4
        return remote(sum_out.at[j], sum_in.at[m], sum_send.at[j], sum_recv.at[m], 2 * (1 - p) + j // 2)

    def total_in(m):
        return remote(sum_out.at[m], sum_in.at[m], sum_send.at[m], sum_recv.at[m], across)

    def own(t):
        return remote(own_out.at[t], own_in.at[t], own_send.at[t], own_recv.at[t], partner)

    small = [pltpu.make_async_copy(a, b, load_sem.at[4 + n]) for n, (a, b) in enumerate(
        [(gain, gain_s), (base_cos, bc_s), (base_sin, bs_s), (step_cos, sc_s), (step_sin, ss_s)])]
    small[0].start()

    def x_rows(n, first):
        at = pl.multiple_of(PAIR * n + CHUNK * (c if first else 1 - c), CHUNK)
        return pl.ds(at, CHUNK)

    x_loads = [pltpu.make_async_copy(x.at[x_rows(n, first), :], x_s.at[x_rows(n, first), :], load_sem.at[2 * n + 1 - first])
               for n in range(2) for first in (1, 0)]
    for load in x_loads:
        load.start()
    w_loads = [pltpu.make_async_copy(a, b, w_sem.at[n]) for n, (a, b) in enumerate([(wk, wk_s), (wv, wv_s), (wq, wq_s), (wo, wo_s)])]
    for load in small[1:] + w_loads:
        load.start()

    barrier = pltpu.get_barrier_semaphore()
    for to in (partner, across, 2 * (1 - p) + 1 - c):
        pl.semaphore_signal(barrier, inc=1, device_id={"tp": to}, device_id_type=MESH)

    def norm(n, first):
        x_loads[2 * n + 1 - first].wait()
        wide = x_s[x_rows(n, first), :].astype(f32)
        scale = lax.rsqrt(jnp.mean(wide * wide, -1, keepdims=True) + 1e-6)
        at = pl.multiple_of(start + PAIR * n + CHUNK * (c if first else 1 - c), CHUNK)
        xn_s[pl.ds(at, CHUNK), :] = (wide * scale * gain_s[...].reshape(1, WIDE).astype(f32)).astype(bf16)

    small[0].wait()
    for n in range(2):
        norm(n, 1)
        if n == 0:
            pl.semaphore_wait(barrier, 3)

        @pl.when(c == 0)
        def _():
            link(n).start()

        norm(n, 0)
        near(n).start()

    near_in(0).wait_recv()

    @pl.when(c == 1)
    def _():
        link(0).start()

    @pl.when(c == 0)
    def _():
        link(2).start()

    near_in(1).wait_recv()

    @pl.when(c == 1)
    def _():
        link(1).start()
        link(2).start()

    link(3).start()

    for load in small[1:] + w_loads[:3]:
        load.wait()
    v_s[:, HEAD:, :] = jnp.ones((KV, 8, ROWS), bf16)
    gap_s[...] = lax.rem(lax.broadcasted_iota(jnp.int32, (PAIR, COLS), 1), PAIR) - lax.broadcasted_iota(jnp.int32, (PAIR, COLS), 0)

    def project(g, slot):
        cos, sin = sc_s[pl.ds(g, 1), :], ss_s[pl.ds(g, 1), :]
        cos_s[...] = bc_s[...] * cos - bs_s[...] * sin
        sin_s[...] = bs_s[...] * cos + bc_s[...] * sin
        at = pl.multiple_of(g * PAIR, PAIR)
        _project(xn_s.at[pl.ds(at, PAIR), :], wq_s, wk_s, wv_s, cos_s, sin_s, q_s.at[slot], k_s, v_s, at)

    def blocks(slot, first, n, size):
        def body(b, _):
            _block(q_s.at[slot], k_s, v_s, top_s.at[slot], mix_s.at[slot], pl.multiple_of(first + b * size, PAIR), size)
        lax.fori_loop(0, n, body, None)

    def causal(slot, first, n):
        top_s[slot] = jnp.full((KV, COLS), NEG, f32)
        mix_s[slot] = jnp.zeros((KV, HEAD + 8, COLS), f32)
        blocks(slot, first, n // 2, 2 * PAIR)
        blocks(slot, first + (n // 2) * 2 * PAIR, n % 2, PAIR)
        _block(q_s.at[slot], k_s, v_s, top_s.at[slot], mix_s.at[slot], pl.multiple_of(first + n * PAIR, PAIR), PAIR, gap_s[...] >= 0)

    def out(dst, at, n):
        for w in range(0, WIDE, 256):
            r = jnp.dot(seen_s[pl.ds(at, n), :], wo_s[:, w : w + 256], preferred_element_type=f32)
            dst[:, w : w + 256] = r.astype(dst.dtype)

    @pl.loop(0, 4)
    def _(t):
        i = (2 * c + t) % 4
        project(4 * p + i, i)

    link_in(0).wait_recv()
    forward(0).start()

    @pl.loop(0, 4)
    def _(i):
        causal(i, mine, i)

    w_loads[3].wait()

    def send_total(j):
        term(j).wait_recv()
        sum_out[j] = (hold_s[j % 2] + term_in[j].astype(f32)).astype(bf16)
        total(j).start()

    @pl.loop(0, 4)
    def _(j):
        g = 4 * (1 - p) + j
        forward_in(j).wait_recv()
        project(g, 4)
        causal(4, 0, g)
        _finish(mix_s.at[4], seen_s)

        @pl.when(j > 0)
        def _():
            send_total(j - 1)

        @pl.when(j < 3)
        def _():
            link_in(j + 1).wait_recv()
            forward(j + 1).start()

        out(term_out.at[j], pl.multiple_of(CHUNK * (1 - c), CHUNK), CHUNK)
        term(j).start()
        out(hold_s.at[j % 2], pl.multiple_of(CHUNK * c, CHUNK), CHUNK)

    send_total(3)

    @pl.loop(0, 4)
    def _(t):
        i = (2 * (1 - c) + t) % 4
        blocks(i, 0, 2 * p, 2 * PAIR)
        _finish(mix_s.at[i], seen_s)
        out(own_s.at[t % 2], 0, PAIR)

        @pl.when(t < 2)
        def _():
            own_out[t] = own_s[t].astype(bf16)
            own(t).start()

    for t in range(2):
        own(t).wait_recv()
        own_s[t] = own_s[t] + x_s[t * PAIR : (t + 1) * PAIR, :].astype(f32) + own_in[t].astype(f32)

    stores = []
    for m in range(4):
        here = slice(m * CHUNK, (m + 1) * CHUNK)
        total_in(m).wait_recv()
        x_s[here, :] = (own_s[m // 2, (m % 2) * CHUNK : (m % 2 + 1) * CHUNK, :] + sum_in[m].astype(f32)).astype(bf16)
        stores.append(pltpu.make_async_copy(x_s.at[here, :], y.at[here, :], y_sem.at[m]))
        stores[-1].start()

    for k in range(2):
        near(k).wait_send()
        own(k).wait_send()
    for j in range(4):
        link(j).wait_send()
        forward(j).wait_send()
        term(j).wait_send()
        total(j).wait_send()
    for store in stores:
        store.wait()


def _tables():
    half = HEAD // 2
    rate = THETA ** (-np.arange(half, dtype=np.float64) / half)
    sign = np.repeat([-1.0, 1.0], half)

    def pair(places):
        angle = np.concatenate([places[:, None] * rate] * 2, axis=1)
        return np.cos(angle).astype(np.float32), (np.sin(angle) * sign).astype(np.float32)

    return [*pair(np.arange(PAIR, dtype=np.float64)), *pair(np.arange(0, ROWS, PAIR, dtype=np.float64))]


def solution(mesh):
    def step(x, gain, wq, wk, wv, wo):
        vmem, dma = pltpu.VMEM, lambda n: pltpu.SemaphoreType.DMA((n,))
        return pl.pallas_call(
            _kernel,
            out_shape=jax.ShapeDtypeStruct((512, WIDE), bf16),
            in_specs=[pl.BlockSpec(memory_space=pl.ANY)] * 10,
            out_specs=pl.BlockSpec(memory_space=pl.ANY),
            scratch_shapes=[
                vmem((512, WIDE), bf16), vmem((WIDE,), bf16),
                vmem((WIDE, 1024), bf16), vmem((WIDE, 512), bf16), vmem((WIDE, 512), bf16), vmem((1024, WIDE), bf16),
                vmem((PAIR, HEAD), f32), vmem((PAIR, HEAD), f32), vmem((8, HEAD), f32), vmem((8, HEAD), f32),
                vmem((PAIR, HEAD), f32), vmem((PAIR, HEAD), f32),
                vmem((ROWS, WIDE), bf16), vmem((5, KV, COLS, HEAD), bf16), vmem((KV, ROWS, HEAD), bf16), vmem((KV, HEAD + 8, ROWS), bf16),
                vmem((5, KV, COLS), f32), vmem((5, KV, HEAD + 8, COLS), f32), vmem((PAIR, COLS), jnp.int32), vmem((PAIR, 1024), bf16),
                vmem((2, CHUNK, WIDE), f32),
                vmem((4, CHUNK, WIDE), bf16), vmem((4, CHUNK, WIDE), bf16), vmem((4, CHUNK, WIDE), bf16), vmem((4, CHUNK, WIDE), bf16),
                vmem((2, PAIR, WIDE), f32), vmem((2, PAIR, WIDE), bf16), vmem((2, PAIR, WIDE), bf16),
                dma(9), dma(4), dma(2), dma(2), dma(4), dma(4), dma(4), dma(4),
                dma(4), dma(4), dma(4), dma(4), dma(2), dma(2), dma(4),
            ],
            compiler_params=pltpu.CompilerParams(collective_id=0, has_side_effects=True, vmem_limit_bytes=VMEM),
        )(x, gain, wq, wk, wv, wo, *map(jnp.asarray, _tables()))

    tokens, columns = P(("dp", "tp"), None), P(None, "tp")
    return jax.shard_map(
        step,
        mesh=mesh,
        in_specs=(tokens, P(None), columns, columns, columns, P("tp", None)),
        out_specs=tokens,
        check_vma=False,
    )
```

```python
import functools

import jax
import jax.numpy as jnp
import numpy as np
from jax import lax
from jax.experimental import pallas as pl
from jax.experimental.pallas import tpu as pltpu
from jax.sharding import PartitionSpec as P

HEAD = 128
THETA = 10000
NEG = -1e30
HIDDEN = 2 * NEG
SCALE2 = HEAD**-0.5 * 1.4426950408889634
ROWS, WIDE = 2048, 2048
PAIR, CHUNK = 256, 128
KV = 4
COLS = 2 * PAIR
VMEM = 61 * 2**20
FIRST, LAST = 32, 32
MESH = pl.DeviceIdType.MESH
bf16, f32 = jnp.bfloat16, jnp.float32


def _dot(a, b, ca, cb):
    return lax.dot_general(a, b, (((ca,), (cb,)), ((), ())), preferred_element_type=f32)


def _turned(t, cos, sin):
    wide = t.astype(bf16).astype(f32)
    return (wide * cos + pltpu.roll(wide, HEAD // 2, 1) * sin).astype(bf16)


def _project(xs, wq, wk, wv, cos, sin, q_dst, k_s, v_s, at):
    here = pl.ds(at, PAIR)
    for n in range(KV // 2):
        r = jnp.dot(xs[...], wk[:, n * 256 : (n + 1) * 256], preferred_element_type=f32)
        for i in range(2):
            k_s[2 * n + i, here, :] = _turned(r[:, i * HEAD : (i + 1) * HEAD], cos[...], sin[...])
    for n in range(KV // 2):
        r = jnp.dot(xs[...], wv[:, n * 256 : (n + 1) * 256], preferred_element_type=f32).astype(bf16)
        for i in range(2):
            v_s[2 * n + i, :HEAD, here] = r[:, i * HEAD : (i + 1) * HEAD].T
    for n in range(KV):
        r = jnp.dot(xs[...], wq[:, n * 256 : (n + 1) * 256], preferred_element_type=f32)
        for i in range(2):
            q_dst[n, i * PAIR : (i + 1) * PAIR, :] = _turned(r[:, i * HEAD : (i + 1) * HEAD], cos[...], sin[...])


def _block(q, k_s, v_s, top_s, miy, at, size, ok=None):
    here = pl.ds(at, size)
    scores = [_dot(k_s[i, here, :], q[i], 1, 1) for i in range(KV)]
    weights, keeps = [], []
    for i, s in enumerate(scores):
        if ok is not None:
            s = jnp.where(ok, s, HIDDEN)
        old = top_s[i : i + 1, :]
        top = jnp.maximum(old, s.max(axis=0, keepdims=True))
        top_s[i : i + 1, :] = top
        weights.append(jnp.exp2((s - top) * SCALE2).astype(bf16))
        keeps.append(jnp.exp2((old - top) * SCALE2))
    for i, (w, keep) in enumerate(zip(weights, keeps)):
        miy[i] = miy[i] * keep + _dot(v_s[i, :, here], w, 1, 0)


def _finish(miy, seen_s):
    for i in range(KV):
        o = (miy[i, :HEAD, :] * (1 / miy[i, HEAD : HEAD + 1, :])).astype(bf16).T
        for n in range(2):
            seen_s[:, (2 * i + n) * HEAD : (2 * i + n + 1) * HEAD] = o[n * PAIR : (n + 1) * PAIR, :]


def _kernel(x, gain, wq, wk, wv, wo, base_cos, base_sin, step_cos, step_sin, y,
            gain_s, wq_s, wk_s, wv_s, wo_s, bc_s, bs_s, sc_s, ss_s, cos_s, sin_s,
            xn_s, q_s, k_s, v_s, top_s, miy, gap_s, seen_s,
            hold_s, term_out, term_in, sum_out, sum_in, own_s, own_out, own_in,
            load_sem, w_sem, near_send, near_recv, link_send, link_recv, fwd_send, fwd_recv,
            term_send, term_recv, sum_send, sum_recv, own_send, own_recv):
    me = lax.axis_index("tp")
    p, c = me // 2, me % 2
    partner, across = 2 * p + 1 - c, 2 * (1 - p) + c
    mine, theirs = 1024 * p, 1024 * (1 - p)
    start = mine + 512 * c

    def remote(src, dst, send, recv, to):
        return pltpu.make_async_remote_copy(src_ref=src, dst_ref=dst, send_sem=send, recv_sem=recv, device_id={"tp": to}, device_id_type=MESH)

    def rows(at, n):
        return xn_s.at[pl.ds(pl.multiple_of(at, FIRST), n), :]

    def near(k):
        return remote(rows(start + PAIR * k, PAIR), rows(start + PAIR * k, PAIR), near_send.at[k], near_recv.at[k], partner)

    def near_in(k):
        at = mine + 512 * (1 - c) + PAIR * k
        return remote(rows(at, PAIR), rows(at, PAIR), near_send.at[k], near_recv.at[k], partner)

    def link(j, part, chip=mine):
        at, n = chip + PAIR * j + CHUNK * c + FIRST * part, (FIRST, CHUNK - FIRST)[part]
        return remote(rows(at, n), rows(at, n), link_send.at[j, part], link_recv.at[j, part], across)

    def links(j):
        link(j, 0).start()
        link(j, 1).start()

    def link_in(j):
        link(j, 0, theirs).wait_recv()
        link(j, 1, theirs).wait_recv()

    def forward(j):
        at = theirs + PAIR * j + CHUNK * c
        return remote(rows(at, CHUNK), rows(at, CHUNK), fwd_send.at[j], fwd_recv.at[j], partner)

    def forward_in(j):
        at = theirs + PAIR * j + CHUNK * (1 - c)
        return remote(rows(at, CHUNK), rows(at, CHUNK), fwd_send.at[j], fwd_recv.at[j], partner)

    def term(j):
        return remote(term_out.at[j], term_in.at[j], term_send.at[j], term_recv.at[j], partner)

    piece = (pl.ds(0, CHUNK - LAST), pl.ds(CHUNK - LAST, LAST))

    def total(j, part):
        m = (2 * j + c) % 4
        return remote(sum_out.at[j, piece[part], :], sum_in.at[m, piece[part], :], sum_send.at[j, part], sum_recv.at[m, part], 2 * (1 - p) + j // 2)

    def total_in(m, part):
        return remote(sum_out.at[m, piece[part], :], sum_in.at[m, piece[part], :], sum_send.at[m, part], sum_recv.at[m, part], across)

    def own(t):
        return remote(own_out.at[t], own_in.at[t], own_send.at[t], own_recv.at[t], partner)

    barrier = pltpu.get_barrier_semaphore()
    for to in (partner, across, 2 * (1 - p) + 1 - c):
        pl.semaphore_signal(barrier, inc=1, device_id={"tp": to}, device_id_type=MESH)

    own_rows = [(CHUNK * c, FIRST), (CHUNK * c + FIRST, CHUNK - FIRST), (CHUNK * (1 - c), CHUNK), (PAIR + CHUNK * c, CHUNK), (PAIR + CHUNK * (1 - c), CHUNK)]
    own_rows = [pl.ds(pl.multiple_of(at, FIRST), n) for at, n in own_rows]
    x_loads = [pltpu.make_async_copy(x.at[here, :], y.at[here, :], load_sem.at[n]) for n, here in enumerate(own_rows)]
    small = [pltpu.make_async_copy(a, b, load_sem.at[5 + n]) for n, (a, b) in enumerate(
        [(gain, gain_s), (base_cos, bc_s), (base_sin, bs_s), (step_cos, sc_s), (step_sin, ss_s)])]
    w_loads = [pltpu.make_async_copy(a, b, w_sem.at[n]) for n, (a, b) in enumerate([(wk, wk_s), (wv, wv_s), (wq, wq_s), (wo, wo_s)])]
    for load in (x_loads[0], small[0], *x_loads[1:]):
        load.start()

    def norm(n):
        x_loads[n].wait()
        wide = y[own_rows[n], :].astype(f32)
        scale = lax.rsqrt(jnp.mean(wide * wide, -1, keepdims=True) + 1e-6)
        at = pl.multiple_of(start + own_rows[n].start, FIRST)
        xn_s[pl.ds(at, own_rows[n].size), :] = (wide * scale * gain_s[...].reshape(1, WIDE).astype(f32)).astype(bf16)

    small[0].wait()
    norm(0)
    pl.semaphore_wait(barrier, 3)
    link(2 * c, 0).start()
    for load in small[1:] + w_loads:
        load.start()
    norm(1)

    @pl.when(c == 0)
    def _():
        link(0, 1).start()

    norm(2)
    near(0).start()
    norm(3)

    @pl.when(c == 0)
    def _():
        links(1)

    norm(4)
    near(1).start()

    near_in(0).wait_recv()

    @pl.when(c == 0)
    def _():
        links(2)

    @pl.when(c == 1)
    def _():
        links(0)

    near_in(1).wait_recv()

    @pl.when(c == 1)
    def _():
        links(1)
        link(2, 1).start()

    links(3)

    for load in small[1:] + w_loads[:3]:
        load.wait()
    v_s[:, HEAD:, :] = jnp.ones((KV, 8, ROWS), bf16)
    gap_s[...] = lax.rem(lax.broadcasted_iota(jnp.int32, (PAIR, COLS), 1), PAIR) - lax.broadcasted_iota(jnp.int32, (PAIR, COLS), 0)

    def project(g, slot):
        cos, sin = sc_s[pl.ds(g, 1), :], ss_s[pl.ds(g, 1), :]
        cos_s[...] = bc_s[...] * cos - bs_s[...] * sin
        sin_s[...] = bs_s[...] * cos + bc_s[...] * sin
        at = pl.multiple_of(g * PAIR, PAIR)
        _project(xn_s.at[pl.ds(at, PAIR), :], wq_s, wk_s, wv_s, cos_s, sin_s, q_s.at[slot], k_s, v_s, at)

    def blocks(slot, first, n, size):
        def body(b, _):
            _block(q_s.at[slot], k_s, v_s, top_s.at[slot], miy.at[slot], pl.multiple_of(first + b * size, PAIR), size)
        lax.fori_loop(0, n, body, None)

    def causal(slot, first, n):
        top_s[slot] = jnp.full((KV, COLS), NEG, f32)
        miy[slot] = jnp.zeros((KV, HEAD + 8, COLS), f32)
        blocks(slot, first, n // 2, 2 * PAIR)
        blocks(slot, first + (n // 2) * 2 * PAIR, n % 2, PAIR)
        _block(q_s.at[slot], k_s, v_s, top_s.at[slot], miy.at[slot], pl.multiple_of(first + n * PAIR, PAIR), PAIR, gap_s[...] >= 0)

    def out(dst, at, n):
        for w in range(0, WIDE, 256):
            r = jnp.dot(seen_s[pl.ds(at, n), :], wo_s[:, w : w + 256], preferred_element_type=f32)
            dst[:, w : w + 256] = r.astype(dst.dtype)

    @pl.loop(0, 4)
    def _(t):
        i = (2 * c + t) % 4
        project(4 * p + i, i)

    link_in(0)
    forward(0).start()

    @pl.loop(0, 4)
    def _(i):
        causal(i, mine, i)

    w_loads[3].wait()

    def send_total(j):
        term(j).wait_recv()
        sum_out[j] = (hold_s[j % 2] + term_in[j].astype(f32)).astype(bf16)
        total(j, 0).start()
        total(j, 1).start()

    @pl.loop(0, 4)
    def _(j):
        g = 4 * (1 - p) + j
        forward_in(j).wait_recv()
        project(g, 4)
        causal(4, 0, g)
        _finish(miy.at[4], seen_s)

        @pl.when(j > 0)
        def _():
            send_total(j - 1)

        @pl.when(j < 3)
        def _():
            link_in(j + 1)
            forward(j + 1).start()

        out(term_out.at[j], pl.multiple_of(CHUNK * (1 - c), CHUNK), CHUNK)
        term(j).start()
        out(hold_s.at[j % 2], pl.multiple_of(CHUNK * c, CHUNK), CHUNK)

    send_total(3)

    @pl.loop(0, 4)
    def _(t):
        i = (2 * (1 - c) + t) % 4
        blocks(i, 0, 2 * p, 2 * PAIR)
        _finish(miy.at[i], seen_s)
        out(own_s.at[t % 2], 0, PAIR)

        @pl.when(t < 2)
        def _():
            own_out[t] = own_s[t].astype(bf16)
            own(t).start()

    for t in range(2):
        own(t).wait_recv()
        own_s[t] = own_s[t] + y[t * PAIR : (t + 1) * PAIR, :].astype(f32) + own_in[t].astype(f32)

    for m, part in ((0, 0), (0, 1), (1, 0), (1, 1), (2, 0), (3, 0), (2, 1), (3, 1)):
        total_in(m, part).wait_recv()
        at, n = piece[part].start, piece[part].size
        y[pl.ds(CHUNK * m + at, n), :] = (own_s[m // 2, pl.ds(CHUNK * (m % 2) + at, n), :] + sum_in[m, pl.ds(at, n), :].astype(f32)).astype(bf16)

    for k in range(2):
        near(k).wait_send()
        own(k).wait_send()
    for j in range(4):
        forward(j).wait_send()
        term(j).wait_send()
        for part in range(2):
            link(j, part).wait_send()
            total(j, part).wait_send()


def _tables():
    half = HEAD // 2
    rate = THETA ** (-np.arange(half, dtype=np.float64) / half)
    sign = np.repeat([-1.0, 1.0], half)

    def pair(places):
        angle = np.concatenate([places[:, None] * rate] * 2, axis=1)
        return np.cos(angle).astype(np.float32), (np.sin(angle) * sign).astype(np.float32)

    return [*pair(np.arange(PAIR, dtype=np.float64)), *pair(np.arange(0, ROWS, PAIR, dtype=np.float64))]


def solution(mesh):
    def step(x, gain, wq, wk, wv, wo):
        vmem, dma = pltpu.VMEM, lambda *n: pltpu.SemaphoreType.DMA(n)
        return pl.pallas_call(
            _kernel,
            out_shape=pltpu.VMEM((512, WIDE), bf16),
            in_specs=[pl.BlockSpec(memory_space=pl.ANY)] * 10,
            out_specs=pl.BlockSpec(memory_space=pltpu.VMEM),
            scratch_shapes=[
                vmem((WIDE,), bf16),
                vmem((WIDE, 1024), bf16), vmem((WIDE, 512), bf16), vmem((WIDE, 512), bf16), vmem((1024, WIDE), bf16),
                vmem((PAIR, HEAD), f32), vmem((PAIR, HEAD), f32), vmem((8, HEAD), f32), vmem((8, HEAD), f32),
                vmem((PAIR, HEAD), f32), vmem((PAIR, HEAD), f32),
                vmem((ROWS, WIDE), bf16), vmem((5, KV, COLS, HEAD), bf16), vmem((KV, ROWS, HEAD), bf16), vmem((KV, HEAD + 8, ROWS), bf16),
                vmem((5, KV, COLS), f32), vmem((5, KV, HEAD + 8, COLS), f32), vmem((PAIR, COLS), jnp.int32), vmem((PAIR, 1024), bf16),
                vmem((2, CHUNK, WIDE), f32),
                vmem((4, CHUNK, WIDE), bf16), vmem((4, CHUNK, WIDE), bf16), vmem((4, CHUNK, WIDE), bf16), vmem((4, CHUNK, WIDE), bf16),
                vmem((2, PAIR, WIDE), f32), vmem((2, PAIR, WIDE), bf16), vmem((2, PAIR, WIDE), bf16),
                dma(10), dma(4), dma(2), dma(2), dma(4, 2), dma(4, 2), dma(4), dma(4),
                dma(4), dma(4), dma(4, 2), dma(4, 2), dma(2), dma(2),
            ],
            compiler_params=pltpu.CompilerParams(collective_id=0, has_side_effects=True, vmem_limit_bytes=VMEM),
        )(x, gain, wq, wk, wv, wo, *map(jnp.asarray, _tables()))

    tokens, columns = P(("dp", "tp"), None), P(None, "tp")
    return jax.shard_map(
        step,
        mesh=mesh,
        in_specs=(tokens, P(None), columns, columns, columns, P("tp", None)),
        out_specs=tokens,
        check_vma=False,
    )
```

```python
import functools

import jax
import jax.numpy as jnp
import numpy as np
from jax import lax
from jax.experimental import pallas as pl
from jax.experimental.pallas import tpu as pltpu
from jax.sharding import PartitionSpec as P

HEAD = 128
THETA = 10000
NEG = -1e30
HIDDEN = 2 * NEG
SCALE2 = HEAD**-0.5 * 1.4426950408889634
ROWS, WIDE = 2048, 2048
PAIR, CHUNK = 256, 128
KV = 4
COLS = 2 * PAIR
VMEM = 61 * 2**20
FIRST, LAST = 32, 32
MESH = pl.DeviceIdType.MESH
bf16, f32 = jnp.bfloat16, jnp.float32


def _dot(a, b, ca, cb):
    return lax.dot_general(a, b, (((ca,), (cb,)), ((), ())), preferred_element_type=f32)


def _turned(t, cos, sin):
    wide = t.astype(bf16).astype(f32)
    return (wide * cos + pltpu.roll(wide, HEAD // 2, 1) * sin).astype(bf16)


def _project(xs, wq, wk, wv, cos, sin, q_dst, k_s, v_s, at):
    here = pl.ds(at, PAIR)
    for n in range(KV // 2):
        r = jnp.dot(xs[...], wk[:, n * 256 : (n + 1) * 256], preferred_element_type=f32)
        for i in range(2):
            k_s[2 * n + i, here, :] = _turned(r[:, i * HEAD : (i + 1) * HEAD], cos[...], sin[...])
    for n in range(KV // 2):
        r = jnp.dot(xs[...], wv[:, n * 256 : (n + 1) * 256], preferred_element_type=f32).astype(bf16)
        for i in range(2):
            v_s[2 * n + i, :HEAD, here] = r[:, i * HEAD : (i + 1) * HEAD].T
    for n in range(KV):
        r = jnp.dot(xs[...], wq[:, n * 256 : (n + 1) * 256], preferred_element_type=f32)
        for i in range(2):
            q_dst[n, i * PAIR : (i + 1) * PAIR, :] = _turned(r[:, i * HEAD : (i + 1) * HEAD], cos[...], sin[...])


def _block(q, k_s, v_s, top_s, mix_s, at, size, ok=None):
    here = pl.ds(at, size)
    scores = [_dot(k_s[i, here, :], q[i], 1, 1) for i in range(KV)]
    weights, keeps = [], []
    for i, s in enumerate(scores):
        if ok is not None:
            s = jnp.where(ok, s, HIDDEN)
        old = top_s[i : i + 1, :]
        top = jnp.maximum(old, s.max(axis=0, keepdims=True))
        top_s[i : i + 1, :] = top
        weights.append(jnp.exp2((s - top) * SCALE2).astype(bf16))
        keeps.append(jnp.exp2((old - top) * SCALE2))
    for i, (w, keep) in enumerate(zip(weights, keeps)):
        mix_s[i] = mix_s[i] * keep + _dot(v_s[i, :, here], w, 1, 0)


def _finish(mix_s, seen_s):
    for i in range(KV):
        o = (mix_s[i, :HEAD, :] * (1 / mix_s[i, HEAD : HEAD + 1, :])).astype(bf16).T
        for n in range(2):
            seen_s[:, (2 * i + n) * HEAD : (2 * i + n + 1) * HEAD] = o[n * PAIR : (n + 1) * PAIR, :]


def _kernel(x, gain, wq, wk, wv, wo, base_cos, base_sin, step_cos, step_sin, y,
            gain_s, wq_s, wk_s, wv_s, wo_s, bc_s, bs_s, sc_s, ss_s, cos_s, sin_s,
            xn_s, q_s, k_s, v_s, top_s, mix_s, gap_s, seen_s,
            hold_s, term_out, term_in, sum_out, sum_in, own_s, own_out, own_in,
            load_sem, w_sem, near_send, near_recv, link_send, link_recv, fwd_send, fwd_recv,
            term_send, term_recv, sum_send, sum_recv, own_send, own_recv):
    me = lax.axis_index("tp")
    p, c = me // 2, me % 2
    partner, across = 2 * p + 1 - c, 2 * (1 - p) + c
    mine, theirs = 1024 * p, 1024 * (1 - p)
    start = mine + 512 * c

    def remote(src, dst, send, recv, to):
        return pltpu.make_async_remote_copy(src_ref=src, dst_ref=dst, send_sem=send, recv_sem=recv, device_id={"tp": to}, device_id_type=MESH)

    def rows(at, n):
        return xn_s.at[pl.ds(pl.multiple_of(at, FIRST), n), :]

    def near(k):
        return remote(rows(start + PAIR * k, PAIR), rows(start + PAIR * k, PAIR), near_send.at[k], near_recv.at[k], partner)

    def near_in(k):
        at = mine + 512 * (1 - c) + PAIR * k
        return remote(rows(at, PAIR), rows(at, PAIR), near_send.at[k], near_recv.at[k], partner)

    def link(j, part=None, chip=mine):
        first, n, sem = {None: (0, CHUNK, 0), 0: (0, FIRST, 0), 1: (FIRST, CHUNK - FIRST, 1)}[part]
        at = chip + PAIR * j + CHUNK * c + first
        return remote(rows(at, n), rows(at, n), link_send.at[j, sem], link_recv.at[j, sem], across)

    def each_link(j, do, chip=mine):
        @pl.when(j == 2 * c)
        def _():
            do(link(j, 0, chip))
            do(link(j, 1, chip))

        @pl.when(j != 2 * c)
        def _():
            do(link(j, None, chip))

    def link_in(j):
        each_link(j, lambda copy: copy.wait_recv(), theirs)

    def forward(j):
        at = theirs + PAIR * j + CHUNK * c
        return remote(rows(at, CHUNK), rows(at, CHUNK), fwd_send.at[j], fwd_recv.at[j], partner)

    def forward_in(j):
        at = theirs + PAIR * j + CHUNK * (1 - c)
        return remote(rows(at, CHUNK), rows(at, CHUNK), fwd_send.at[j], fwd_recv.at[j], partner)

    def term(j):
        return remote(term_out.at[j], term_in.at[j], term_send.at[j], term_recv.at[j], partner)

    piece = (pl.ds(0, CHUNK - LAST), pl.ds(CHUNK - LAST, LAST), pl.ds(0, CHUNK))

    def total(j, part=2):
        m = (2 * j + c) % 4
        return remote(sum_out.at[j, piece[part], :], sum_in.at[m, piece[part], :], sum_send.at[j, part % 2], sum_recv.at[m, part % 2], 2 * (1 - p) + j // 2)

    def total_in(m, part):
        return remote(sum_out.at[m, piece[part], :], sum_in.at[m, piece[part], :], sum_send.at[m, part % 2], sum_recv.at[m, part % 2], across)

    def own(t):
        return remote(own_out.at[t], own_in.at[t], own_send.at[t], own_recv.at[t], partner)

    barrier = pltpu.get_barrier_semaphore()
    for to in (partner, across, 2 * (1 - p) + 1 - c):
        pl.semaphore_signal(barrier, inc=1, device_id={"tp": to}, device_id_type=MESH)

    own_rows = [(CHUNK * c, FIRST), (CHUNK * c + FIRST, CHUNK - FIRST), (CHUNK * (1 - c), CHUNK), (PAIR + CHUNK * c, CHUNK), (PAIR + CHUNK * (1 - c), CHUNK)]
    own_rows = [pl.ds(pl.multiple_of(at, FIRST), n) for at, n in own_rows]
    x_loads = [pltpu.make_async_copy(x.at[here, :], y.at[here, :], load_sem.at[n]) for n, here in enumerate(own_rows)]
    small = [pltpu.make_async_copy(a, b, load_sem.at[5 + n]) for n, (a, b) in enumerate(
        [(gain, gain_s), (base_cos, bc_s), (base_sin, bs_s), (step_cos, sc_s), (step_sin, ss_s)])]
    w_loads = [pltpu.make_async_copy(a, b, w_sem.at[n]) for n, (a, b) in enumerate([(wk, wk_s), (wv, wv_s), (wq, wq_s), (wo, wo_s)])]
    for load in (x_loads[0], small[0], *x_loads[1:]):
        load.start()

    def norm(n):
        x_loads[n].wait()
        wide = y[own_rows[n], :].astype(f32)
        scale = lax.rsqrt(jnp.mean(wide * wide, -1, keepdims=True) + 1e-6)
        at = pl.multiple_of(start + own_rows[n].start, FIRST)
        xn_s[pl.ds(at, own_rows[n].size), :] = (wide * scale * gain_s[...].reshape(1, WIDE).astype(f32)).astype(bf16)

    small[0].wait()
    norm(0)
    pl.semaphore_wait(barrier, 3)
    link(2 * c, 0).start()
    for load in small[1:] + w_loads:
        load.start()
    norm(1)

    @pl.when(c == 0)
    def _():
        link(0, 1).start()

    norm(2)
    near(0).start()
    norm(3)

    @pl.when(c == 0)
    def _():
        link(1).start()

    norm(4)
    near(1).start()

    near_in(0).wait_recv()

    @pl.when(c == 0)
    def _():
        link(2).start()

    @pl.when(c == 1)
    def _():
        link(0).start()

    near_in(1).wait_recv()

    @pl.when(c == 1)
    def _():
        link(1).start()
        link(2, 1).start()

    link(3).start()

    for load in small[1:] + w_loads[:3]:
        load.wait()
    v_s[:, HEAD:, :] = jnp.ones((KV, 8, ROWS), bf16)
    gap_s[...] = lax.rem(lax.broadcasted_iota(jnp.int32, (PAIR, COLS), 1), PAIR) - lax.broadcasted_iota(jnp.int32, (PAIR, COLS), 0)

    def project(g, slot):
        cos, sin = sc_s[pl.ds(g, 1), :], ss_s[pl.ds(g, 1), :]
        cos_s[...] = bc_s[...] * cos - bs_s[...] * sin
        sin_s[...] = bs_s[...] * cos + bc_s[...] * sin
        at = pl.multiple_of(g * PAIR, PAIR)
        _project(xn_s.at[pl.ds(at, PAIR), :], wq_s, wk_s, wv_s, cos_s, sin_s, q_s.at[slot], k_s, v_s, at)

    def attend(slot, g):
        top_s[...] = jnp.full((KV, COLS), NEG, f32)
        mix_s[...] = jnp.zeros((KV, HEAD + 8, COLS), f32)

        def block(at, size, ok=None):
            _block(q_s.at[slot], k_s, v_s, top_s, mix_s, pl.multiple_of(at, PAIR), size, ok)

        lax.fori_loop(0, g // 2, lambda b, _: block(b * 2 * PAIR, 2 * PAIR), None)
        lax.fori_loop(0, g % 2, lambda b, _: block((g - 1) * PAIR, PAIR), None)
        block(g * PAIR, PAIR, gap_s[...] >= 0)
        _finish(mix_s, seen_s)

    def out(dst, at, n):
        for w in range(0, WIDE, 256):
            r = jnp.dot(seen_s[pl.ds(at, n), :], wo_s[:, w : w + 256], preferred_element_type=f32)
            dst[:, w : w + 256] = r.astype(dst.dtype)

    @pl.loop(0, 4)
    def _(t):
        i = (2 * c + t) % 4
        project(4 * p + i, i)

    link_in(0)
    forward(0).start()

    w_loads[3].wait()

    def send_total(j, parts=(2,)):
        term(j).wait_recv()
        sum_out[j] = (hold_s[j % 2] + term_in[j].astype(f32)).astype(bf16)
        for part in parts:
            total(j, part).start()

    @pl.loop(0, 4)
    def _(j):
        g = 4 * (1 - p) + j
        forward_in(j).wait_recv()
        project(g, 4)
        attend(4, g)

        @pl.when(j > 0)
        def _():
            send_total(j - 1)

        @pl.when(j < 3)
        def _():
            link_in(j + 1)
            forward(j + 1).start()

        out(term_out.at[j], pl.multiple_of(CHUNK * (1 - c), CHUNK), CHUNK)
        term(j).start()
        out(hold_s.at[j % 2], pl.multiple_of(CHUNK * c, CHUNK), CHUNK)

    send_total(3, (0, 1))

    @pl.loop(0, 4)
    def _(t):
        i = (2 * (1 - c) + t) % 4
        attend(i, 4 * p + i)
        out(own_s.at[t % 2], 0, PAIR)

        @pl.when(t < 2)
        def _():
            own_out[t] = own_s[t].astype(bf16)
            own(t).start()

    for t in range(2):
        own(t).wait_recv()
        own_s[t] = own_s[t] + y[t * PAIR : (t + 1) * PAIR, :].astype(f32) + own_in[t].astype(f32)

    def finished(m, part):
        total_in(m, part).wait_recv()
        at, n = piece[part].start, piece[part].size
        y[pl.ds(CHUNK * m + at, n), :] = (own_s[m // 2, pl.ds(CHUNK * (m % 2) + at, n), :] + sum_in[m, pl.ds(at, n), :].astype(f32)).astype(bf16)

    finished(0, 2)
    finished(1, 2)

    @pl.when(c == 0)
    def _():
        finished(2, 2)
        finished(3, 2)

    @pl.when(c == 1)
    def _():
        for part in range(2):
            finished(2, part)
            finished(3, part)

    for k in range(2):
        near(k).wait_send()
        own(k).wait_send()
    for j in range(4):
        forward(j).wait_send()
        term(j).wait_send()
        each_link(j, lambda copy: copy.wait_send())
        for part in (0, 1) if j == 3 else (2,):
            total(j, part).wait_send()


def _tables():
    half = HEAD // 2
    rate = THETA ** (-np.arange(half, dtype=np.float64) / half)
    sign = np.repeat([-1.0, 1.0], half)

    def pair(places):
        angle = np.concatenate([places[:, None] * rate] * 2, axis=1)
        return np.cos(angle).astype(np.float32), (np.sin(angle) * sign).astype(np.float32)

    return [*pair(np.arange(PAIR, dtype=np.float64)), *pair(np.arange(0, ROWS, PAIR, dtype=np.float64))]


def solution(mesh):
    def step(x, gain, wq, wk, wv, wo):
        vmem, dma = pltpu.VMEM, lambda *n: pltpu.SemaphoreType.DMA(n)
        return pl.pallas_call(
            _kernel,
            out_shape=pltpu.VMEM((512, WIDE), bf16),
            in_specs=[pl.BlockSpec(memory_space=pl.ANY)] * 10,
            out_specs=pl.BlockSpec(memory_space=pltpu.VMEM),
            scratch_shapes=[
                vmem((WIDE,), bf16),
                vmem((WIDE, 1024), bf16), vmem((WIDE, 512), bf16), vmem((WIDE, 512), bf16), vmem((1024, WIDE), bf16),
                vmem((PAIR, HEAD), f32), vmem((PAIR, HEAD), f32), vmem((8, HEAD), f32), vmem((8, HEAD), f32),
                vmem((PAIR, HEAD), f32), vmem((PAIR, HEAD), f32),
                vmem((ROWS, WIDE), bf16), vmem((5, KV, COLS, HEAD), bf16), vmem((KV, ROWS, HEAD), bf16), vmem((KV, HEAD + 8, ROWS), bf16),
                vmem((KV, COLS), f32), vmem((KV, HEAD + 8, COLS), f32), vmem((PAIR, COLS), jnp.int32), vmem((PAIR, 1024), bf16),
                vmem((2, CHUNK, WIDE), f32),
                vmem((4, CHUNK, WIDE), bf16), vmem((4, CHUNK, WIDE), bf16), vmem((4, CHUNK, WIDE), bf16), vmem((4, CHUNK, WIDE), bf16),
                vmem((2, PAIR, WIDE), f32), vmem((2, PAIR, WIDE), bf16), vmem((2, PAIR, WIDE), bf16),
                dma(10), dma(4), dma(2), dma(2), dma(4, 2), dma(4, 2), dma(4), dma(4),
                dma(4), dma(4), dma(4, 2), dma(4, 2), dma(2), dma(2),
            ],
            compiler_params=pltpu.CompilerParams(collective_id=0, has_side_effects=True, vmem_limit_bytes=VMEM),
        )(x, gain, wq, wk, wv, wo, *map(jnp.asarray, _tables()))

    tokens, columns = P(("dp", "tp"), None), P(None, "tp")
    return jax.shard_map(
        step,
        mesh=mesh,
        in_specs=(tokens, P(None), columns, columns, columns, P("tp", None)),
        out_specs=tokens,
        check_vma=False,
    )
```

```python
import functools

import jax
import jax.numpy as jnp
import numpy as np
from jax import lax
from jax.experimental import pallas as pl
from jax.experimental.pallas import tpu as pltpu
from jax.sharding import PartitionSpec as P

HEAD = 128
THETA = 10000
NEG = float("-inf")
SCALE2 = HEAD**-0.5 * 1.4426950408889634
ROWS, WIDE = 2048, 2048
PAIR, CHUNK = 256, 128
KV = 4
COLS = 2 * PAIR
VMEM = 61 * 2**20
FIRST, LAST = 32, 32
MESH = pl.DeviceIdType.MESH
bf16, f32 = jnp.bfloat16, jnp.float32


def _dot(a, b, ca, cb):
    return lax.dot_general(a, b, (((ca,), (cb,)), ((), ())), preferred_element_type=f32)


def _turned(t, cos, sin):
    wide = t.astype(bf16).astype(f32)
    return (wide * cos + pltpu.roll(wide, HEAD // 2, 1) * sin).astype(bf16)


def _project(xs, wq, wk, wv, cos, sin, q_dst, k_s, v_s, at):
    here = pl.ds(at, PAIR)
    for n in range(KV // 2):
        r = jnp.dot(xs[...], wk[:, n * 256 : (n + 1) * 256], preferred_element_type=f32)
        for i in range(2):
            k_s[2 * n + i, here, :] = _turned(r[:, i * HEAD : (i + 1) * HEAD], cos[...], sin[...])
    for n in range(KV // 2):
        r = jnp.dot(xs[...], wv[:, n * 256 : (n + 1) * 256], preferred_element_type=f32).astype(bf16)
        for i in range(2):
            v_s[2 * n + i, :HEAD, here] = r[:, i * HEAD : (i + 1) * HEAD].T
    for n in range(KV):
        r = jnp.dot(xs[...], wq[:, n * 256 : (n + 1) * 256], preferred_element_type=f32)
        for i in range(2):
            q_dst[n, i * PAIR : (i + 1) * PAIR, :] = _turned(r[:, i * HEAD : (i + 1) * HEAD], cos[...], sin[...])


def _block(q, k_s, v_s, top_s, mix_s, at, size, ok=None):
    here = pl.ds(at, size)
    scores = [_dot(k_s[i, here, :], q[i], 1, 1) for i in range(KV)]
    weights, keeps = [], []
    for i, s in enumerate(scores):
        if ok is not None:
            s = jnp.where(ok, s, NEG)
        old = top_s[i : i + 1, :]
        top = jnp.maximum(old, s.max(axis=0, keepdims=True))
        top_s[i : i + 1, :] = top
        weights.append(jnp.exp2((s - top) * SCALE2).astype(bf16))
        keeps.append(jnp.exp2((old - top) * SCALE2))
    for i, (w, keep) in enumerate(zip(weights, keeps)):
        mix_s[i] = mix_s[i] * keep + _dot(v_s[i, :, here], w, 1, 0)


def _finish(mix_s, seen_s):
    for i in range(KV):
        o = (mix_s[i, :HEAD, :] * (1 / mix_s[i, HEAD : HEAD + 1, :])).astype(bf16).T
        for n in range(2):
            seen_s[:, (2 * i + n) * HEAD : (2 * i + n + 1) * HEAD] = o[n * PAIR : (n + 1) * PAIR, :]


def _kernel(x, gain, wq, wk, wv, wo, base_cos, base_sin, step_cos, step_sin, y,
            gain_s, raw_s, wq_s, wk_s, wv_s, wo_s, bc_s, bs_s, sc_s, ss_s, cos_s, sin_s,
            xn_s, q_s, k_s, v_s, top_s, mix_s, gap_s, seen_s,
            hold_s, term_out, term_in, sum_out, sum_in, own_s, own_out, own_in,
            load_sem, w_sem, near_send, near_recv, link_send, link_recv, fwd_send, fwd_recv,
            term_send, term_recv, sum_send, sum_recv, own_send, own_recv):
    me = lax.axis_index("tp")
    p, c = me // 2, me % 2
    partner, across = 2 * p + 1 - c, 2 * (1 - p) + c
    mine, theirs = 1024 * p, 1024 * (1 - p)
    start = mine + 512 * c

    own_rows = [(CHUNK * c, FIRST), (CHUNK * c + FIRST, CHUNK - FIRST), (CHUNK * (1 - c), CHUNK), (PAIR + CHUNK * c, CHUNK), (PAIR + CHUNK * (1 - c), CHUNK)]
    own_rows = [pl.ds(pl.multiple_of(at, FIRST), n) for at, n in own_rows]

    def remote(src, dst, send, recv, to):
        return pltpu.make_async_remote_copy(src_ref=src, dst_ref=dst, send_sem=send, recv_sem=recv, device_id={"tp": to}, device_id_type=MESH)

    def rows(at, n):
        return xn_s.at[pl.ds(pl.multiple_of(at, FIRST), n), :]

    def near(k):
        return remote(rows(start + PAIR * k, PAIR), rows(start + PAIR * k, PAIR), near_send.at[k], near_recv.at[k], partner)

    def near_in(k):
        at = mine + 512 * (1 - c) + PAIR * k
        return remote(rows(at, PAIR), rows(at, PAIR), near_send.at[k], near_recv.at[k], partner)

    def link(j, part=None, chip=mine):
        first, n, sem = {None: (0, CHUNK, 0), 0: (0, FIRST, 0), 1: (FIRST, CHUNK - FIRST, 1)}[part]
        at = chip + PAIR * j + CHUNK * c + first
        if part == 0:
            return remote(x.at[own_rows[0], :], raw_s, link_send.at[j, sem], link_recv.at[j, sem], across)
        return remote(rows(at, n), rows(at, n), link_send.at[j, sem], link_recv.at[j, sem], across)

    def each_link(j, do, chip=mine):
        @pl.when(j == 2 * c)
        def _():
            do(link(j, 0, chip))
            do(link(j, 1, chip))

        @pl.when(j != 2 * c)
        def _():
            do(link(j, None, chip))

    def link_in(j):
        each_link(j, lambda copy: copy.wait_recv(), theirs)

        @pl.when(j == 2 * c)
        def _():
            xn_s[pl.ds(pl.multiple_of(theirs + PAIR * j + CHUNK * c, FIRST), FIRST), :] = normed(raw_s[...])

    def forward(j):
        at = theirs + PAIR * j + CHUNK * c
        return remote(rows(at, CHUNK), rows(at, CHUNK), fwd_send.at[j], fwd_recv.at[j], partner)

    def forward_in(j):
        at = theirs + PAIR * j + CHUNK * (1 - c)
        return remote(rows(at, CHUNK), rows(at, CHUNK), fwd_send.at[j], fwd_recv.at[j], partner)

    def term(j):
        return remote(term_out.at[j], term_in.at[j], term_send.at[j], term_recv.at[j], partner)

    piece = (pl.ds(0, CHUNK - LAST), pl.ds(CHUNK - LAST, LAST), pl.ds(0, CHUNK))

    def total(j, part=2):
        m = (2 * j + c) % 4
        return remote(sum_out.at[j, piece[part], :], sum_in.at[m, piece[part], :], sum_send.at[j, part % 2], sum_recv.at[m, part % 2], 2 * (1 - p) + j // 2)

    def total_in(m, part):
        return remote(sum_out.at[m, piece[part], :], sum_in.at[m, piece[part], :], sum_send.at[m, part % 2], sum_recv.at[m, part % 2], across)

    def own(t):
        return remote(own_out.at[t], own_in.at[t], own_send.at[t], own_recv.at[t], partner)

    barrier = pltpu.get_barrier_semaphore()
    for to in (partner, across, 2 * (1 - p) + 1 - c):
        pl.semaphore_signal(barrier, inc=1, device_id={"tp": to}, device_id_type=MESH)

    x_loads = [pltpu.make_async_copy(x.at[here, :], y.at[here, :], load_sem.at[n]) for n, here in enumerate(own_rows)]
    small = [pltpu.make_async_copy(a, b, load_sem.at[5 + n]) for n, (a, b) in enumerate(
        [(gain, gain_s), (base_cos, bc_s), (base_sin, bs_s), (step_cos, sc_s), (step_sin, ss_s)])]
    w_loads = [pltpu.make_async_copy(a, b, w_sem.at[n]) for n, (a, b) in enumerate([(wk, wk_s), (wv, wv_s), (wq, wq_s), (wo, wo_s)])]
    for load in (x_loads[0], small[0], *x_loads[1:]):
        load.start()

    def normed(t):
        wide = t.astype(f32)
        scale = lax.rsqrt(jnp.mean(wide * wide, -1, keepdims=True) + 1e-6)
        return (wide * scale * gain_s[...].reshape(1, WIDE).astype(f32)).astype(bf16)

    def norm(n):
        x_loads[n].wait()
        xn_s[pl.ds(pl.multiple_of(start + own_rows[n].start, FIRST), own_rows[n].size), :] = normed(y[own_rows[n], :])

    pl.semaphore_wait(barrier, 3)
    link(2 * c, 0).start()
    small[0].wait()
    norm(0)
    for load in small[1:] + w_loads:
        load.start()
    norm(1)

    @pl.when(c == 0)
    def _():
        link(0, 1).start()

    norm(2)
    near(0).start()
    norm(3)

    @pl.when(c == 0)
    def _():
        link(1).start()

    norm(4)
    near(1).start()

    near_in(0).wait_recv()

    @pl.when(c == 0)
    def _():
        link(2).start()

    @pl.when(c == 1)
    def _():
        link(0).start()

    near_in(1).wait_recv()

    @pl.when(c == 1)
    def _():
        link(1).start()
        link(2, 1).start()

    link(3).start()

    for load in small[1:] + w_loads[:3]:
        load.wait()
    v_s[:, HEAD:, :] = jnp.ones((KV, 8, ROWS), bf16)
    gap_s[...] = lax.rem(lax.broadcasted_iota(jnp.int32, (PAIR, COLS), 1), PAIR) - lax.broadcasted_iota(jnp.int32, (PAIR, COLS), 0)

    def project(g, slot):
        cos, sin = sc_s[pl.ds(g, 1), :], ss_s[pl.ds(g, 1), :]
        cos_s[...] = bc_s[...] * cos - bs_s[...] * sin
        sin_s[...] = bs_s[...] * cos + bc_s[...] * sin
        at = pl.multiple_of(g * PAIR, PAIR)
        _project(xn_s.at[pl.ds(at, PAIR), :], wq_s, wk_s, wv_s, cos_s, sin_s, q_s.at[slot], k_s, v_s, at)

    def attend(slot, g):
        top_s[...] = jnp.full((KV, COLS), NEG, f32)
        mix_s[...] = jnp.zeros((KV, HEAD + 8, COLS), f32)

        def block(at, size, ok=None):
            _block(q_s.at[slot], k_s, v_s, top_s, mix_s, pl.multiple_of(at, PAIR), size, ok)

        lax.fori_loop(0, g // 2, lambda b, _: block(b * 2 * PAIR, 2 * PAIR), None)
        lax.fori_loop(0, g % 2, lambda b, _: block((g - 1) * PAIR, PAIR), None)
        block(g * PAIR, PAIR, gap_s[...] >= 0)
        _finish(mix_s, seen_s)

    def out(dst, at, n):
        for w in range(0, WIDE, 256):
            r = jnp.dot(seen_s[pl.ds(at, n), :], wo_s[:, w : w + 256], preferred_element_type=f32)
            dst[:, w : w + 256] = r.astype(dst.dtype)

    @pl.loop(0, 4)
    def _(t):
        i = (2 * c + t) % 4
        project(4 * p + i, i)

    link_in(0)
    forward(0).start()

    w_loads[3].wait()

    def send_total(j, parts=(2,)):
        term(j).wait_recv()
        sum_out[j] = (hold_s[j % 2] + term_in[j].astype(f32)).astype(bf16)
        for part in parts:
            total(j, part).start()

    @pl.loop(0, 4)
    def _(j):
        g = 4 * (1 - p) + j
        forward_in(j).wait_recv()
        project(g, 4)
        attend(4, g)

        @pl.when(j > 0)
        def _():
            send_total(j - 1)

        @pl.when(j < 3)
        def _():
            link_in(j + 1)
            forward(j + 1).start()

        out(term_out.at[j], pl.multiple_of(CHUNK * (1 - c), CHUNK), CHUNK)
        term(j).start()
        out(hold_s.at[j % 2], pl.multiple_of(CHUNK * c, CHUNK), CHUNK)

    send_total(3, (0, 1))

    @pl.loop(0, 4)
    def _(t):
        i = (2 * (1 - c) + t) % 4
        attend(i, 4 * p + i)
        out(own_s.at[t % 2], 0, PAIR)

        @pl.when(t < 2)
        def _():
            own_out[t] = own_s[t].astype(bf16)
            own(t).start()

    for t in range(2):
        own(t).wait_recv()
        own_s[t] = own_s[t] + y[t * PAIR : (t + 1) * PAIR, :].astype(f32) + own_in[t].astype(f32)

    def finished(m, part):
        total_in(m, part).wait_recv()
        at, n = piece[part].start, piece[part].size
        y[pl.ds(CHUNK * m + at, n), :] = (own_s[m // 2, pl.ds(CHUNK * (m % 2) + at, n), :] + sum_in[m, pl.ds(at, n), :].astype(f32)).astype(bf16)

    finished(0, 2)
    finished(1, 2)

    @pl.when(c == 0)
    def _():
        finished(2, 2)
        finished(3, 2)

    @pl.when(c == 1)
    def _():
        for part in range(2):
            finished(2, part)
            finished(3, part)

    for k in range(2):
        near(k).wait_send()
        own(k).wait_send()
    for j in range(4):
        forward(j).wait_send()
        term(j).wait_send()
        each_link(j, lambda copy: copy.wait_send())
        for part in (0, 1) if j == 3 else (2,):
            total(j, part).wait_send()


def _tables():
    half = HEAD // 2
    rate = THETA ** (-np.arange(half, dtype=np.float64) / half)
    sign = np.repeat([-1.0, 1.0], half)

    def pair(places):
        angle = np.concatenate([places[:, None] * rate] * 2, axis=1)
        return np.cos(angle).astype(np.float32), (np.sin(angle) * sign).astype(np.float32)

    return [*pair(np.arange(PAIR, dtype=np.float64)), *pair(np.arange(0, ROWS, PAIR, dtype=np.float64))]


def solution(mesh):
    def step(x, gain, wq, wk, wv, wo):
        vmem, dma = pltpu.VMEM, lambda *n: pltpu.SemaphoreType.DMA(n)
        return pl.pallas_call(
            _kernel,
            out_shape=pltpu.VMEM((512, WIDE), bf16),
            in_specs=[pl.BlockSpec(memory_space=pl.ANY)] * 10,
            out_specs=pl.BlockSpec(memory_space=pltpu.VMEM),
            scratch_shapes=[
                vmem((WIDE,), bf16), vmem((FIRST, WIDE), bf16),
                vmem((WIDE, 1024), bf16), vmem((WIDE, 512), bf16), vmem((WIDE, 512), bf16), vmem((1024, WIDE), bf16),
                vmem((PAIR, HEAD), f32), vmem((PAIR, HEAD), f32), vmem((8, HEAD), f32), vmem((8, HEAD), f32),
                vmem((PAIR, HEAD), f32), vmem((PAIR, HEAD), f32),
                vmem((ROWS, WIDE), bf16), vmem((5, KV, COLS, HEAD), bf16), vmem((KV, ROWS, HEAD), bf16), vmem((KV, HEAD + 8, ROWS), bf16),
                vmem((KV, COLS), f32), vmem((KV, HEAD + 8, COLS), f32), vmem((PAIR, COLS), jnp.int32), vmem((PAIR, 1024), bf16),
                vmem((2, CHUNK, WIDE), f32),
                vmem((4, CHUNK, WIDE), bf16), vmem((4, CHUNK, WIDE), bf16), vmem((4, CHUNK, WIDE), bf16), vmem((4, CHUNK, WIDE), bf16),
                vmem((2, PAIR, WIDE), f32), vmem((2, PAIR, WIDE), bf16), vmem((2, PAIR, WIDE), bf16),
                dma(10), dma(4), dma(2), dma(2), dma(4, 2), dma(4, 2), dma(4), dma(4),
                dma(4), dma(4), dma(4, 2), dma(4, 2), dma(2), dma(2),
            ],
            compiler_params=pltpu.CompilerParams(collective_id=0, has_side_effects=True, vmem_limit_bytes=VMEM),
        )(x, gain, wq, wk, wv, wo, *map(jnp.asarray, _tables()))

    tokens, columns = P(("dp", "tp"), None), P(None, "tp")
    return jax.shard_map(
        step,
        mesh=mesh,
        in_specs=(tokens, P(None), columns, columns, columns, P("tp", None)),
        out_specs=tokens,
        check_vma=False,
    )
```

```python
import functools

import jax
import jax.numpy as jnp
import numpy as np
from jax import lax
from jax.experimental import pallas as pl
from jax.experimental.pallas import tpu as pltpu
from jax.sharding import PartitionSpec as P

HEAD = 128
THETA = 10000
NEG = float("-inf")
SCALE2 = HEAD**-0.5 * 1.4426950408889634
ROWS, WIDE = 2048, 2048
PAIR, CHUNK = 256, 128
KV = 4
COLS = 2 * PAIR
VMEM = 61 * 2**20
FIRST, LAST = 96, 32
ALIGN = 16
MESH = pl.DeviceIdType.MESH
bf16, f32 = jnp.bfloat16, jnp.float32


def _dot(a, b, ca, cb):
    return lax.dot_general(a, b, (((ca,), (cb,)), ((), ())), preferred_element_type=f32)


def _turned(t, cos, sin):
    wide = t.astype(bf16).astype(f32)
    return (wide * cos + pltpu.roll(wide, HEAD // 2, 1) * sin).astype(bf16)


def _project(xs, wq, wk, wv, cos, sin, q_dst, k_s, v_s, at):
    here = pl.ds(at, PAIR)
    for n in range(KV // 2):
        r = jnp.dot(xs[...], wk[:, n * 256 : (n + 1) * 256], preferred_element_type=f32)
        for i in range(2):
            k_s[2 * n + i, here, :] = _turned(r[:, i * HEAD : (i + 1) * HEAD], cos[...], sin[...])
    for n in range(KV // 2):
        r = jnp.dot(xs[...], wv[:, n * 256 : (n + 1) * 256], preferred_element_type=f32).astype(bf16)
        for i in range(2):
            v_s[2 * n + i, :HEAD, here] = r[:, i * HEAD : (i + 1) * HEAD].T
    for n in range(KV):
        r = jnp.dot(xs[...], wq[:, n * 256 : (n + 1) * 256], preferred_element_type=f32)
        for i in range(2):
            q_dst[n, i * PAIR : (i + 1) * PAIR, :] = _turned(r[:, i * HEAD : (i + 1) * HEAD], cos[...], sin[...])


def _block(q, k_s, v_s, top_s, mix_s, at, size, ok=None):
    here = pl.ds(at, size)
    scores = [_dot(k_s[i, here, :], q[i], 1, 1) for i in range(KV)]
    weights, keeps = [], []
    for i, s in enumerate(scores):
        if ok is not None:
            s = jnp.where(ok, s, NEG)
        old = top_s[i : i + 1, :]
        top = jnp.maximum(old, s.max(axis=0, keepdims=True))
        top_s[i : i + 1, :] = top
        weights.append(jnp.exp2((s - top) * SCALE2).astype(bf16))
        keeps.append(jnp.exp2((old - top) * SCALE2))
    for i, (w, keep) in enumerate(zip(weights, keeps)):
        mix_s[i] = mix_s[i] * keep + _dot(v_s[i, :, here], w, 1, 0)


def _finish(mix_s, seen_s):
    for i in range(KV):
        o = (mix_s[i, :HEAD, :] * (1 / mix_s[i, HEAD : HEAD + 1, :])).astype(bf16).T
        for n in range(2):
            seen_s[:, (2 * i + n) * HEAD : (2 * i + n + 1) * HEAD] = o[n * PAIR : (n + 1) * PAIR, :]


def _kernel(x, gain, wq, wk, wv, wo, base_cos, base_sin, step_cos, step_sin, y,
            gain_s, raw_s, wq_s, wk_s, wv_s, wo_s, bc_s, bs_s, sc_s, ss_s, cos_s, sin_s,
            xn_s, q_s, k_s, v_s, top_s, mix_s, gap_s, seen_s,
            hold_s, term_out, term_in, sum_out, sum_in, own_s, own_out, own_in,
            load_sem, w_sem, near_send, near_recv, link_send, link_recv, fwd_send, fwd_recv,
            term_send, term_recv, sum_send, sum_recv, own_send, own_recv, met_sem):
    me = lax.axis_index("tp")
    p, c = me // 2, me % 2
    partner, across = 2 * p + 1 - c, 2 * (1 - p) + c
    mine, theirs = 1024 * p, 1024 * (1 - p)
    start = mine + 512 * c

    own_rows = [(CHUNK * c, FIRST), (CHUNK * c + FIRST, CHUNK - FIRST), (CHUNK * (1 - c), CHUNK), (PAIR + CHUNK * c, CHUNK), (PAIR + CHUNK * (1 - c), CHUNK)]
    own_rows = [pl.ds(pl.multiple_of(at, ALIGN), n) for at, n in own_rows]

    def remote(src, dst, send, recv, to):
        return pltpu.make_async_remote_copy(src_ref=src, dst_ref=dst, send_sem=send, recv_sem=recv, device_id={"tp": to}, device_id_type=MESH)

    def rows(at, n):
        return xn_s.at[pl.ds(pl.multiple_of(at, ALIGN), n), :]

    def near(k):
        return remote(rows(start + PAIR * k, PAIR), rows(start + PAIR * k, PAIR), near_send.at[k], near_recv.at[k], partner)

    def near_in(k):
        at = mine + 512 * (1 - c) + PAIR * k
        return remote(rows(at, PAIR), rows(at, PAIR), near_send.at[k], near_recv.at[k], partner)

    def link(j, part=None, chip=mine):
        first, n, sem = {None: (0, CHUNK, 0), 0: (0, FIRST, 0), 1: (FIRST, CHUNK - FIRST, 1)}[part]
        at = chip + PAIR * j + CHUNK * c + first
        if part == 0:
            return remote(x.at[own_rows[0], :], raw_s, link_send.at[j, sem], link_recv.at[j, sem], across)
        return remote(rows(at, n), rows(at, n), link_send.at[j, sem], link_recv.at[j, sem], across)

    def each_link(j, do, chip=mine):
        @pl.when(j == 2 * c)
        def _():
            do(link(j, 0, chip))
            do(link(j, 1, chip))

        @pl.when(j != 2 * c)
        def _():
            do(link(j, None, chip))

    def link_in(j):
        each_link(j, lambda copy: copy.wait_recv(), theirs)

        @pl.when(j == 2 * c)
        def _():
            xn_s[pl.ds(pl.multiple_of(theirs + PAIR * j + CHUNK * c, ALIGN), FIRST), :] = normed(raw_s[...])

    def forward(j):
        at = theirs + PAIR * j + CHUNK * c
        return remote(rows(at, CHUNK), rows(at, CHUNK), fwd_send.at[j], fwd_recv.at[j], partner)

    def forward_in(j):
        at = theirs + PAIR * j + CHUNK * (1 - c)
        return remote(rows(at, CHUNK), rows(at, CHUNK), fwd_send.at[j], fwd_recv.at[j], partner)

    def term(j):
        return remote(term_out.at[j], term_in.at[j], term_send.at[j], term_recv.at[j], partner)

    piece = (pl.ds(0, CHUNK - LAST), pl.ds(CHUNK - LAST, LAST), pl.ds(0, CHUNK))

    def total(j, part=2):
        m = (2 * j + c) % 4
        return remote(sum_out.at[j, piece[part], :], sum_in.at[m, piece[part], :], sum_send.at[j, part % 2], sum_recv.at[m, part % 2], 2 * (1 - p) + j // 2)

    def total_in(m, part):
        return remote(sum_out.at[m, piece[part], :], sum_in.at[m, piece[part], :], sum_send.at[m, part % 2], sum_recv.at[m, part % 2], across)

    def own(t):
        return remote(own_out.at[t], own_in.at[t], own_send.at[t], own_recv.at[t], partner)

    barrier = pltpu.get_barrier_semaphore()
    even = 1 - (p + c) % 2
    after, before = even * partner + (1 - even) * across, even * across + (1 - even) * partner
    pl.semaphore_signal(barrier, inc=1, device_id={"tp": after}, device_id_type=MESH)

    x_loads = [pltpu.make_async_copy(x.at[here, :], y.at[here, :], load_sem.at[n]) for n, here in enumerate(own_rows)]
    small = [pltpu.make_async_copy(a, b, load_sem.at[5 + n]) for n, (a, b) in enumerate(
        [(gain, gain_s), (base_cos, bc_s), (base_sin, bs_s), (step_cos, sc_s), (step_sin, ss_s)])]
    w_loads = [pltpu.make_async_copy(a, b, w_sem.at[n]) for n, (a, b) in enumerate([(wk, wk_s), (wv, wv_s), (wq, wq_s), (wo, wo_s)])]
    for load in (x_loads[0], small[0], *x_loads[1:]):
        load.start()

    def normed(t):
        wide = t.astype(f32)
        scale = lax.rsqrt(jnp.mean(wide * wide, -1, keepdims=True) + 1e-6)
        return (wide * scale * gain_s[...].reshape(1, WIDE).astype(f32)).astype(bf16)

    def norm(n):
        x_loads[n].wait()
        xn_s[pl.ds(pl.multiple_of(start + own_rows[n].start, ALIGN), own_rows[n].size), :] = normed(y[own_rows[n], :])

    pl.semaphore_wait(barrier, 1)
    pl.semaphore_signal(met_sem, inc=1, device_id={"tp": before}, device_id_type=MESH)

    @pl.when(even == 1)
    def _():
        link(2 * c, 0).start()

    @pl.when(even == 0)
    def _():
        pl.semaphore_wait(met_sem, 1)
        link(2 * c, 0).start()

    small[0].wait()
    norm(0)
    for load in small[1:] + w_loads:
        load.start()
    norm(1)

    @pl.when(c == 0)
    def _():
        link(0, 1).start()

    norm(2)

    @pl.when(even == 1)
    def _():
        pl.semaphore_wait(met_sem, 1)

    near(0).start()
    norm(3)

    @pl.when(c == 0)
    def _():
        link(1).start()

    norm(4)
    near(1).start()

    near_in(0).wait_recv()

    @pl.when(c == 0)
    def _():
        link(2).start()

    @pl.when(c == 1)
    def _():
        link(0).start()

    near_in(1).wait_recv()

    @pl.when(c == 1)
    def _():
        link(1).start()
        link(2, 1).start()

    link(3).start()

    for load in small[1:] + w_loads[:3]:
        load.wait()
    v_s[:, HEAD:, :] = jnp.ones((KV, 8, ROWS), bf16)
    gap_s[...] = lax.rem(lax.broadcasted_iota(jnp.int32, (PAIR, COLS), 1), PAIR) - lax.broadcasted_iota(jnp.int32, (PAIR, COLS), 0)

    def project(g, slot):
        cos, sin = sc_s[pl.ds(g, 1), :], ss_s[pl.ds(g, 1), :]
        cos_s[...] = bc_s[...] * cos - bs_s[...] * sin
        sin_s[...] = bs_s[...] * cos + bc_s[...] * sin
        at = pl.multiple_of(g * PAIR, PAIR)
        _project(xn_s.at[pl.ds(at, PAIR), :], wq_s, wk_s, wv_s, cos_s, sin_s, q_s.at[slot], k_s, v_s, at)

    def attend(slot, g):
        top_s[...] = jnp.full((KV, COLS), NEG, f32)
        mix_s[...] = jnp.zeros((KV, HEAD + 8, COLS), f32)

        def block(at, size, ok=None):
            _block(q_s.at[slot], k_s, v_s, top_s, mix_s, pl.multiple_of(at, PAIR), size, ok)

        lax.fori_loop(0, g // 2, lambda b, _: block(b * 2 * PAIR, 2 * PAIR), None)
        lax.fori_loop(0, g % 2, lambda b, _: block((g - 1) * PAIR, PAIR), None)
        block(g * PAIR, PAIR, gap_s[...] >= 0)
        _finish(mix_s, seen_s)

    def out(dst, at, n):
        for w in range(0, WIDE, 256):
            r = jnp.dot(seen_s[pl.ds(at, n), :], wo_s[:, w : w + 256], preferred_element_type=f32)
            dst[:, w : w + 256] = r.astype(dst.dtype)

    @pl.loop(0, 4)
    def _(t):
        i = (2 * c + t) % 4
        project(4 * p + i, i)

    link_in(0)
    forward(0).start()

    w_loads[3].wait()

    def send_total(j, parts=(2,)):
        term(j).wait_recv()
        sum_out[j] = (hold_s[j % 2] + term_in[j].astype(f32)).astype(bf16)
        for part in parts:
            total(j, part).start()

    @pl.loop(0, 4)
    def _(j):
        g = 4 * (1 - p) + j
        forward_in(j).wait_recv()
        project(g, 4)
        attend(4, g)

        @pl.when(j > 0)
        def _():
            send_total(j - 1)

        @pl.when(j < 3)
        def _():
            link_in(j + 1)
            forward(j + 1).start()

        out(term_out.at[j], pl.multiple_of(CHUNK * (1 - c), CHUNK), CHUNK)
        term(j).start()
        out(hold_s.at[j % 2], pl.multiple_of(CHUNK * c, CHUNK), CHUNK)

    send_total(3, (0, 1))

    @pl.loop(0, 4)
    def _(t):
        i = (2 * (1 - c) + t) % 4
        attend(i, 4 * p + i)
        out(own_s.at[t % 2], 0, PAIR)

        @pl.when(t < 2)
        def _():
            own_out[t] = own_s[t].astype(bf16)
            own(t).start()

    for t in range(2):
        own(t).wait_recv()
        own_s[t] = own_s[t] + y[t * PAIR : (t + 1) * PAIR, :].astype(f32) + own_in[t].astype(f32)

    def finished(m, part):
        total_in(m, part).wait_recv()
        at, n = piece[part].start, piece[part].size
        y[pl.ds(CHUNK * m + at, n), :] = (own_s[m // 2, pl.ds(CHUNK * (m % 2) + at, n), :] + sum_in[m, pl.ds(at, n), :].astype(f32)).astype(bf16)

    finished(0, 2)
    finished(1, 2)

    @pl.when(c == 0)
    def _():
        finished(2, 2)
        finished(3, 2)

    @pl.when(c == 1)
    def _():
        for part in range(2):
            finished(2, part)
            finished(3, part)

    for k in range(2):
        near(k).wait_send()
        own(k).wait_send()
    for j in range(4):
        forward(j).wait_send()
        term(j).wait_send()
        each_link(j, lambda copy: copy.wait_send())
        for part in (0, 1) if j == 3 else (2,):
            total(j, part).wait_send()


def _tables():
    half = HEAD // 2
    rate = THETA ** (-np.arange(half, dtype=np.float64) / half)
    sign = np.repeat([-1.0, 1.0], half)

    def pair(places):
        angle = np.concatenate([places[:, None] * rate] * 2, axis=1)
        return np.cos(angle).astype(np.float32), (np.sin(angle) * sign).astype(np.float32)

    return [*pair(np.arange(PAIR, dtype=np.float64)), *pair(np.arange(0, ROWS, PAIR, dtype=np.float64))]


def solution(mesh):
    def step(x, gain, wq, wk, wv, wo):
        vmem, dma = pltpu.VMEM, lambda *n: pltpu.SemaphoreType.DMA(n)
        return pl.pallas_call(
            _kernel,
            out_shape=pltpu.VMEM((512, WIDE), bf16),
            in_specs=[pl.BlockSpec(memory_space=pl.ANY)] * 10,
            out_specs=pl.BlockSpec(memory_space=pltpu.VMEM),
            scratch_shapes=[
                vmem((WIDE,), bf16), vmem((FIRST, WIDE), bf16),
                vmem((WIDE, 1024), bf16), vmem((WIDE, 512), bf16), vmem((WIDE, 512), bf16), vmem((1024, WIDE), bf16),
                vmem((PAIR, HEAD), f32), vmem((PAIR, HEAD), f32), vmem((8, HEAD), f32), vmem((8, HEAD), f32),
                vmem((PAIR, HEAD), f32), vmem((PAIR, HEAD), f32),
                vmem((ROWS, WIDE), bf16), vmem((5, KV, COLS, HEAD), bf16), vmem((KV, ROWS, HEAD), bf16), vmem((KV, HEAD + 8, ROWS), bf16),
                vmem((KV, COLS), f32), vmem((KV, HEAD + 8, COLS), f32), vmem((PAIR, COLS), jnp.int32), vmem((PAIR, 1024), bf16),
                vmem((2, CHUNK, WIDE), f32),
                vmem((4, CHUNK, WIDE), bf16), vmem((4, CHUNK, WIDE), bf16), vmem((4, CHUNK, WIDE), bf16), vmem((4, CHUNK, WIDE), bf16),
                vmem((2, PAIR, WIDE), f32), vmem((2, PAIR, WIDE), bf16), vmem((2, PAIR, WIDE), bf16),
                dma(10), dma(4), dma(2), dma(2), dma(4, 2), dma(4, 2), dma(4), dma(4),
                dma(4), dma(4), dma(4, 2), dma(4, 2), dma(2), dma(2), pltpu.SemaphoreType.REGULAR,
            ],
            compiler_params=pltpu.CompilerParams(collective_id=0, has_side_effects=True, vmem_limit_bytes=VMEM),
        )(x, gain, wq, wk, wv, wo, *map(jnp.asarray, _tables()))

    tokens, columns = P(("dp", "tp"), None), P(None, "tp")
    return jax.shard_map(
        step,
        mesh=mesh,
        in_specs=(tokens, P(None), columns, columns, columns, P("tp", None)),
        out_specs=tokens,
        check_vma=False,
    )
```

```python
import jax
import jax.numpy as jnp
import numpy as np
from jax import lax
from jax.experimental import pallas as pl
from jax.experimental.pallas import tpu as pltpu
from jax.sharding import PartitionSpec as P

HEAD = 128
THETA = 10000
NEG = float("-inf")
SCALE2 = HEAD**-0.5 * 1.4426950408889634
ROWS, WIDE = 2048, 2048
PAIR, CHUNK = 256, 128
KV = 4
COLS = 2 * PAIR
VMEM = 61 * 2**20
FIRST, LAST = 96, 32
ALIGN = 16
MESH = pl.DeviceIdType.MESH
bf16, f32 = jnp.bfloat16, jnp.float32


def _dot(a, b, ca, cb):
    return lax.dot_general(a, b, (((ca,), (cb,)), ((), ())), preferred_element_type=f32)


def _turned(t, cos, sin):
    wide = t.astype(bf16).astype(f32)
    return (wide * cos + pltpu.roll(wide, HEAD // 2, 1) * sin).astype(bf16)


def _project(xs, wq, wk, wv, cos, sin, q_dst, k_s, v_s, at):
    here = pl.ds(at, PAIR)
    for n in range(KV // 2):
        r = jnp.dot(xs[...], wk[:, n * 256 : (n + 1) * 256], preferred_element_type=f32)
        for i in range(2):
            k_s[2 * n + i, here, :] = _turned(r[:, i * HEAD : (i + 1) * HEAD], cos[...], sin[...])
    for n in range(KV // 2):
        r = jnp.dot(xs[...], wv[:, n * 256 : (n + 1) * 256], preferred_element_type=f32).astype(bf16)
        for i in range(2):
            v_s[2 * n + i, :HEAD, here] = r[:, i * HEAD : (i + 1) * HEAD].T
    for n in range(KV):
        r = jnp.dot(xs[...], wq[:, n * 256 : (n + 1) * 256], preferred_element_type=f32)
        for i in range(2):
            q_dst[n, i * PAIR : (i + 1) * PAIR, :] = _turned(r[:, i * HEAD : (i + 1) * HEAD], cos[...], sin[...])


def _block(q, k_s, v_s, top_s, mix_s, at, size, ok=None):
    here = pl.ds(at, size)
    scores = [_dot(k_s[i, here, :], q[i], 1, 1) for i in range(KV)]
    weights, keeps = [], []
    for i, s in enumerate(scores):
        if ok is not None:
            s = jnp.where(ok, s, NEG)
        old = top_s[i : i + 1, :]
        top = jnp.maximum(old, s.max(axis=0, keepdims=True))
        top_s[i : i + 1, :] = top
        weights.append(jnp.exp2((s - top) * SCALE2).astype(bf16))
        keeps.append(jnp.exp2((old - top) * SCALE2))
    for i, (w, keep) in enumerate(zip(weights, keeps)):
        mix_s[i] = mix_s[i] * keep + _dot(v_s[i, :, here], w, 1, 0)


def _finish(mix_s, seen_s):
    for i in range(KV):
        o = (mix_s[i, :HEAD, :] * (1 / mix_s[i, HEAD : HEAD + 1, :])).astype(bf16).T
        for n in range(2):
            seen_s[:, (2 * i + n) * HEAD : (2 * i + n + 1) * HEAD] = o[n * PAIR : (n + 1) * PAIR, :]


def _kernel(x, gain, wq, wk, wv, wo, table, y,
            gain_s, raw_s, wq_s, wk_s, wv_s, wo_s, table_s, cos_s, sin_s,
            xn_s, q_s, k_s, v_s, top_s, mix_s, gap_s, seen_s,
            hold_s, term_out, term_in, sum_out, sum_in, own_s, own_out, own_in,
            load_sem, w_sem, near_send, near_recv, link_send, link_recv, fwd_send, fwd_recv,
            term_send, term_recv, sum_send, sum_recv, own_send, own_recv, met_sem):
    me = lax.axis_index("tp")
    p, c = me // 2, me % 2
    partner, across = 2 * p + 1 - c, 2 * (1 - p) + c
    mine, theirs = 1024 * p, 1024 * (1 - p)
    start = mine + 512 * c

    own_rows = [(CHUNK * c, FIRST), (CHUNK * c + FIRST, CHUNK - FIRST), (CHUNK * (1 - c), CHUNK), (PAIR + CHUNK * c, CHUNK), (PAIR + CHUNK * (1 - c), CHUNK)]
    own_rows = [pl.ds(pl.multiple_of(at, ALIGN), n) for at, n in own_rows]

    def remote(src, dst, send, recv, to):
        return pltpu.make_async_remote_copy(src_ref=src, dst_ref=dst, send_sem=send, recv_sem=recv, device_id={"tp": to}, device_id_type=MESH)

    def rows(at, n):
        return xn_s.at[pl.ds(pl.multiple_of(at, ALIGN), n), :]

    def near(k):
        return remote(rows(start + PAIR * k, PAIR), rows(start + PAIR * k, PAIR), near_send, near_recv.at[k], partner)

    def near_in(k):
        at = mine + 512 * (1 - c) + PAIR * k
        return remote(rows(at, PAIR), rows(at, PAIR), near_send, near_recv.at[k], partner)

    def link(j, part=None, chip=mine):
        first, n, sem = {None: (0, CHUNK, j), 0: (0, FIRST, j), 1: (FIRST, CHUNK - FIRST, 4)}[part]
        at = chip + PAIR * j + CHUNK * c + first
        if part == 0:
            return remote(x.at[own_rows[0], :], raw_s, link_send, link_recv.at[sem], across)
        return remote(rows(at, n), rows(at, n), link_send, link_recv.at[sem], across)

    def each_link(j, do, chip=mine):
        @pl.when(j == 2 * c)
        def _():
            do(link(j, 0, chip))
            do(link(j, 1, chip))

        @pl.when(j != 2 * c)
        def _():
            do(link(j, None, chip))

    def link_in(j):
        each_link(j, lambda copy: copy.wait_recv(), theirs)

        @pl.when(j == 2 * c)
        def _():
            xn_s[pl.ds(pl.multiple_of(theirs + PAIR * j + CHUNK * c, ALIGN), FIRST), :] = normed(raw_s[...])

    def forward(j):
        at = theirs + PAIR * j + CHUNK * c
        return remote(rows(at, CHUNK), rows(at, CHUNK), fwd_send, fwd_recv.at[j % 2], partner)

    def forward_in(j):
        at = theirs + PAIR * j + CHUNK * (1 - c)
        return remote(rows(at, CHUNK), rows(at, CHUNK), fwd_send, fwd_recv.at[j % 2], partner)

    def term(j):
        return remote(term_out.at[j], term_in.at[j], term_send, term_recv.at[j % 2], partner)

    piece = (pl.ds(0, CHUNK - LAST), pl.ds(CHUNK - LAST, LAST), pl.ds(0, CHUNK))

    def total(j, part=2):
        m = (2 * j + c) % 4
        sem = sum_recv.at[2 if part == 1 else j % 2]
        return remote(sum_out.at[j, piece[part], :], sum_in.at[m, piece[part], :], sum_send, sem, 2 * (1 - p) + j // 2)

    def total_in(half, part=2):
        both = pl.ds(2 * half, 2), piece[part]
        return remote(sum_out.at[*both, :], sum_in.at[*both, :], sum_send, sum_recv.at[2 if part == 1 else half], across)

    def own(t):
        return remote(own_out.at[t], own_in.at[t], own_send, own_recv, partner)

    barrier = pltpu.get_barrier_semaphore()
    even = 1 - (p + c) % 2
    after, before = even * partner + (1 - even) * across, even * across + (1 - even) * partner
    pl.semaphore_signal(barrier, inc=1, device_id={"tp": after}, device_id_type=MESH)

    x_loads = [pltpu.make_async_copy(x.at[here, :], y.at[here, :], load_sem.at[n]) for n, here in enumerate(own_rows)]
    small = [pltpu.make_async_copy(a, b, load_sem.at[5 + n]) for n, (a, b) in enumerate(
        [(gain, gain_s), (table, table_s)])]
    w_loads = [pltpu.make_async_copy(a, b, w_sem.at[n]) for n, (a, b) in enumerate([(wk, wk_s), (wv, wv_s), (wq, wq_s), (wo, wo_s)])]
    pl.semaphore_wait(barrier, 1)
    pl.semaphore_signal(met_sem, inc=1, device_id={"tp": before}, device_id_type=MESH)

    @pl.when(even == 1)
    def _():
        link(2 * c, 0).start()

    for load in (x_loads[0], small[0], *x_loads[1:]):
        load.start()

    def normed(t):
        wide = t.astype(f32)
        scale = lax.rsqrt(jnp.mean(wide * wide, -1, keepdims=True) + 1e-6)
        return (wide * scale * gain_s[...].reshape(1, WIDE).astype(f32)).astype(bf16)

    def norm(n):
        x_loads[n].wait()
        xn_s[pl.ds(pl.multiple_of(start + own_rows[n].start, ALIGN), own_rows[n].size), :] = normed(y[own_rows[n], :])

    @pl.when(even == 0)
    def _():
        pl.semaphore_wait(met_sem, 1)
        link(2 * c, 0).start()

    small[0].wait()
    norm(0)
    for load in small[1:] + w_loads:
        load.start()
    norm(1)

    @pl.when(c == 0)
    def _():
        link(0, 1).start()

    norm(2)

    @pl.when(even == 1)
    def _():
        pl.semaphore_wait(met_sem, 1)

    near(0).start()
    norm(3)

    @pl.when(c == 0)
    def _():
        link(1).start()

    norm(4)
    near(1).start()

    near_in(0).wait_recv()

    @pl.when(c == 0)
    def _():
        link(2).start()

    @pl.when(c == 1)
    def _():
        link(0).start()

    near_in(1).wait_recv()

    @pl.when(c == 1)
    def _():
        link(1).start()
        link(2, 1).start()

    link(3).start()

    for load in small[1:] + w_loads[:3]:
        load.wait()
    v_s[:, HEAD:, :] = jnp.ones((KV, 8, ROWS), bf16)
    gap_s[...] = lax.rem(lax.broadcasted_iota(jnp.int32, (PAIR, COLS), 1), PAIR) - lax.broadcasted_iota(jnp.int32, (PAIR, COLS), 0)

    def project(g, slot):
        cos, sin = table_s[pl.ds(2 * PAIR + g, 1), :], table_s[pl.ds(2 * PAIR + 8 + g, 1), :]
        first_cos, first_sin = table_s[:PAIR, :], table_s[PAIR : 2 * PAIR, :]
        cos_s[...] = first_cos * cos - first_sin * sin
        sin_s[...] = first_sin * cos + first_cos * sin
        at = pl.multiple_of(g * PAIR, PAIR)
        _project(xn_s.at[pl.ds(at, PAIR), :], wq_s, wk_s, wv_s, cos_s, sin_s, q_s.at[slot], k_s, v_s, at)

    def attend(slot, g):
        top_s[...] = jnp.full((KV, COLS), NEG, f32)
        mix_s[...] = jnp.zeros((KV, HEAD + 8, COLS), f32)

        def block(at, size, ok=None):
            _block(q_s.at[slot], k_s, v_s, top_s, mix_s, pl.multiple_of(at, PAIR), size, ok)

        lax.fori_loop(0, g // 2, lambda b, _: block(b * 2 * PAIR, 2 * PAIR), None)
        lax.fori_loop(0, g % 2, lambda b, _: block((g - 1) * PAIR, PAIR), None)
        block(g * PAIR, PAIR, gap_s[...] >= 0)
        _finish(mix_s, seen_s)

    def out(dst, at, n):
        for w in range(0, WIDE, 256):
            r = jnp.dot(seen_s[pl.ds(at, n), :], wo_s[:, w : w + 256], preferred_element_type=f32)
            dst[:, w : w + 256] = r.astype(dst.dtype)

    @pl.loop(0, 4)
    def _(t):
        i = (2 * c + t) % 4
        project(4 * p + i, i)

    link_in(0)
    forward(0).start()

    w_loads[3].wait()

    def send_total(j, parts=(2,)):
        term(j).wait_recv()
        sum_out[j] = (hold_s[j % 2] + term_in[j].astype(f32)).astype(bf16)
        for part in parts:
            total(j, part).start()

    @pl.loop(0, 4)
    def _(j):
        g = 4 * (1 - p) + j
        forward_in(j).wait_recv()
        project(g, 4)
        attend(4, g)

        @pl.when(j > 0)
        def _():
            send_total(j - 1)

        @pl.when(j < 3)
        def _():
            link_in(j + 1)
            forward(j + 1).start()

        out(term_out.at[j], pl.multiple_of(CHUNK * (1 - c), CHUNK), CHUNK)
        term(j).start()
        out(hold_s.at[j % 2], pl.multiple_of(CHUNK * c, CHUNK), CHUNK)

    send_total(3, (0, 1))

    @pl.loop(0, 4)
    def _(t):
        i = (2 * (1 - c) + t) % 4
        attend(i, 4 * p + i)
        out(own_s.at[t % 2], 0, PAIR)

        @pl.when(t < 2)
        def _():
            own_out[t] = own_s[t].astype(bf16)
            own(t).start()

    remote(own_out, own_in, own_send, own_recv, partner).wait_recv()
    for t in range(2):
        own_s[t] = own_s[t] + y[t * PAIR : (t + 1) * PAIR, :].astype(f32) + own_in[t].astype(f32)

    def finished(half, part=2):
        total_in(half, part).wait_recv()
        at, n = piece[part].start, piece[part].size
        for i in range(2):
            y[pl.ds(PAIR * half + CHUNK * i + at, n), :] = (
                own_s[half, pl.ds(CHUNK * i + at, n), :] + sum_in[2 * half + i, pl.ds(at, n), :].astype(f32)).astype(bf16)

    finished(0)

    @pl.when(c == 0)
    def _():
        finished(1)

    @pl.when(c == 1)
    def _():
        finished(1, 0)
        finished(1, 1)

    for ref, sent, got in ((rows(start, 512), near_send, near_recv.at[0]), (rows(start, 512), link_send, link_recv.at[0]),
                           (rows(start, 512), fwd_send, fwd_recv.at[0]), (term_out, term_send, term_recv.at[0]),
                           (sum_out, sum_send, sum_recv.at[0]), (own_out, own_send, own_recv)):
        remote(ref, ref, sent, got, partner).wait_send()


def _table():
    half = HEAD // 2
    rate = THETA ** (-np.arange(half, dtype=np.float64) / half)
    sign = np.repeat([-1.0, 1.0], half)

    def pair(places):
        angle = np.concatenate([places[:, None] * rate] * 2, axis=1)
        return np.cos(angle).astype(np.float32), (np.sin(angle) * sign).astype(np.float32)

    return np.concatenate([*pair(np.arange(PAIR, dtype=np.float64)), *pair(np.arange(0, ROWS, PAIR, dtype=np.float64))])


def solution(mesh):
    def step(x, gain, wq, wk, wv, wo):
        vmem, DMA, dma = pltpu.VMEM, pltpu.SemaphoreType.DMA, lambda n: pltpu.SemaphoreType.DMA((n,))
        return pl.pallas_call(
            _kernel,
            out_shape=pltpu.VMEM((512, WIDE), bf16),
            in_specs=[pl.BlockSpec(memory_space=pl.ANY)] * 7,
            out_specs=pl.BlockSpec(memory_space=pltpu.VMEM),
            scratch_shapes=[
                vmem((WIDE,), bf16), vmem((FIRST, WIDE), bf16),
                vmem((WIDE, 1024), bf16), vmem((WIDE, 512), bf16), vmem((WIDE, 512), bf16), vmem((1024, WIDE), bf16),
                vmem((2 * PAIR + 16, HEAD), f32),
                vmem((PAIR, HEAD), f32), vmem((PAIR, HEAD), f32),
                vmem((ROWS, WIDE), bf16), vmem((5, KV, COLS, HEAD), bf16), vmem((KV, ROWS, HEAD), bf16), vmem((KV, HEAD + 8, ROWS), bf16),
                vmem((KV, COLS), f32), vmem((KV, HEAD + 8, COLS), f32), vmem((PAIR, COLS), jnp.int32), vmem((PAIR, 1024), bf16),
                vmem((2, CHUNK, WIDE), f32),
                vmem((4, CHUNK, WIDE), bf16), vmem((4, CHUNK, WIDE), bf16), vmem((4, CHUNK, WIDE), bf16), vmem((4, CHUNK, WIDE), bf16),
                vmem((2, PAIR, WIDE), f32), vmem((2, PAIR, WIDE), bf16), vmem((2, PAIR, WIDE), bf16),
                dma(7), dma(4), DMA, dma(2), DMA, dma(5), DMA, dma(2),
                DMA, dma(2), DMA, dma(3), DMA, DMA, pltpu.SemaphoreType.REGULAR,
            ],
            compiler_params=pltpu.CompilerParams(collective_id=0, has_side_effects=True, vmem_limit_bytes=VMEM),
        )(x, gain, wq, wk, wv, wo, jnp.asarray(_table()))

    tokens, columns = P(("dp", "tp"), None), P(None, "tp")
    return jax.shard_map(
        step,
        mesh=mesh,
        in_specs=(tokens, P(None), columns, columns, columns, P("tp", None)),
        out_specs=tokens,
        check_vma=False,
    )
```

```python
import jax
import jax.numpy as jnp
import numpy as np
from jax import lax
from jax.experimental import pallas as pl
from jax.experimental.pallas import tpu as pltpu
from jax.sharding import PartitionSpec as P

HEAD = 128
THETA = 10000
NEG = float("-inf")
SCALE2 = HEAD**-0.5 * 1.4426950408889634
ROWS, WIDE = 2048, 2048
PAIR, CHUNK = 256, 128
KV = 4
COLS = 2 * PAIR
VMEM = 61 * 2**20
FIRST, LAST = 96, 32
ALIGN = 16
MESH = pl.DeviceIdType.MESH
bf16, f32 = jnp.bfloat16, jnp.float32


def _dot(a, b, ca, cb):
    return lax.dot_general(a, b, (((ca,), (cb,)), ((), ())), preferred_element_type=f32)


def _turned(t, cos, sin):
    wide = t.astype(bf16).astype(f32)
    return (wide * cos + pltpu.roll(wide, HEAD // 2, 1) * sin).astype(bf16)


def _project(xs, wq, wk, wv, cos, sin, q_dst, k_s, v_s, at):
    here = pl.ds(at, PAIR)
    for n in range(KV // 2):
        r = jnp.dot(xs[...], wk[:, n * 256 : (n + 1) * 256], preferred_element_type=f32)
        for i in range(2):
            k_s[2 * n + i, here, :] = _turned(r[:, i * HEAD : (i + 1) * HEAD], cos[...], sin[...])
    for n in range(KV // 2):
        r = jnp.dot(xs[...], wv[:, n * 256 : (n + 1) * 256], preferred_element_type=f32).astype(bf16)
        for i in range(2):
            v_s[2 * n + i, :HEAD, here] = r[:, i * HEAD : (i + 1) * HEAD].T
    for n in range(KV):
        r = jnp.dot(xs[...], wq[:, n * 256 : (n + 1) * 256], preferred_element_type=f32)
        for i in range(2):
            q_dst[n, i * PAIR : (i + 1) * PAIR, :] = _turned(r[:, i * HEAD : (i + 1) * HEAD], cos[...], sin[...])


def _block(q, k_s, v_s, top_s, mix_s, at, size, ok=None):
    here = pl.ds(at, size)
    scores = [_dot(k_s[i, here, :], q[i], 1, 1) for i in range(KV)]
    weights, keeps = [], []
    for i, s in enumerate(scores):
        if ok is not None:
            s = jnp.where(ok, s, NEG)
        old = top_s[i : i + 1, :]
        top = jnp.maximum(old, s.max(axis=0, keepdims=True))
        top_s[i : i + 1, :] = top
        weights.append(jnp.exp2((s - top) * SCALE2).astype(bf16))
        keeps.append(jnp.exp2((old - top) * SCALE2))
    for i, (w, keep) in enumerate(zip(weights, keeps)):
        mix_s[i] = mix_s[i] * keep + _dot(v_s[i, :, here], w, 1, 0)


def _finish(mix_s, seen_s):
    for i in range(KV):
        o = (mix_s[i, :HEAD, :] * (1 / mix_s[i, HEAD : HEAD + 1, :])).astype(bf16).T
        for n in range(2):
            seen_s[:, (2 * i + n) * HEAD : (2 * i + n + 1) * HEAD] = o[n * PAIR : (n + 1) * PAIR, :]


def _kernel(x, gain, wq, wk, wv, wo, table, y,
            gain_s, raw_s, wq_s, wk_s, wv_s, wo_s, table_s, cos_s, sin_s,
            xn_s, q_s, k_s, v_s, top_s, mix_s, gap_s, seen_s,
            hold_s, term_out, term_in, sum_out, sum_in, own_s, own_out, own_in,
            load_sem, w_sem, rows_send, sum_send, near_recv, link_recv, fwd_recv, term_recv, sum_recv, own_recv, met_sem):
    me = lax.axis_index("tp")
    p, c = me // 2, me % 2
    partner, across = 2 * p + 1 - c, 2 * (1 - p) + c
    mine, theirs = 1024 * p, 1024 * (1 - p)
    start = mine + 512 * c

    own_rows = [(CHUNK * c, FIRST), (CHUNK * c + FIRST, CHUNK - FIRST), (CHUNK * (1 - c), CHUNK), (PAIR, PAIR)]
    own_rows = [pl.ds(pl.multiple_of(at, ALIGN), n) for at, n in own_rows]

    def remote(src, dst, send, recv, to):
        return pltpu.make_async_remote_copy(src_ref=src, dst_ref=dst, send_sem=send, recv_sem=recv, device_id={"tp": to}, device_id_type=MESH)

    def rows(at, n):
        return xn_s.at[pl.ds(pl.multiple_of(at, ALIGN), n), :]

    def near(k):
        return remote(rows(start + PAIR * k, PAIR), rows(start + PAIR * k, PAIR), rows_send, near_recv.at[k], partner)

    def near_in(k):
        at = mine + 512 * (1 - c) + PAIR * k
        return remote(rows(at, PAIR), rows(at, PAIR), rows_send, near_recv.at[k], partner)

    def link(j, part=None, chip=mine):
        first, n, sem = {None: (0, CHUNK, j), 0: (0, FIRST, j), 1: (FIRST, CHUNK - FIRST, 4)}[part]
        at = chip + PAIR * j + CHUNK * c + first
        if part == 0:
            return remote(x.at[own_rows[0], :], raw_s, rows_send, link_recv.at[sem], across)
        return remote(rows(at, n), rows(at, n), rows_send, link_recv.at[sem], across)

    def each_link(j, do, chip=mine):
        @pl.when(j == 2 * c)
        def _():
            do(link(j, 0, chip))
            do(link(j, 1, chip))

        @pl.when(j != 2 * c)
        def _():
            do(link(j, None, chip))

    def link_in(j):
        each_link(j, lambda copy: copy.wait_recv(), theirs)

        @pl.when(j == 2 * c)
        def _():
            xn_s[pl.ds(pl.multiple_of(theirs + PAIR * j + CHUNK * c, ALIGN), FIRST), :] = normed(raw_s[...])

    def forward(j):
        at = theirs + PAIR * j + CHUNK * c
        return remote(rows(at, CHUNK), rows(at, CHUNK), rows_send, fwd_recv.at[j % 2], partner)

    def forward_in(j):
        at = theirs + PAIR * j + CHUNK * (1 - c)
        return remote(rows(at, CHUNK), rows(at, CHUNK), rows_send, fwd_recv.at[j % 2], partner)

    def term(j):
        return remote(term_out.at[j], term_in.at[j], rows_send, term_recv.at[j % 2], partner)

    piece = (pl.ds(0, CHUNK - LAST), pl.ds(CHUNK - LAST, LAST), pl.ds(0, CHUNK))

    def total(j, part=2):
        m = (2 * j + c) % 4
        sem = sum_recv.at[2 if part == 1 else j % 2]
        return remote(sum_out.at[j, piece[part], :], sum_in.at[m, piece[part], :], sum_send, sem, 2 * (1 - p) + j // 2)

    def total_in(half, part=2):
        both = pl.ds(2 * half, 2), piece[part]
        return remote(sum_out.at[*both, :], sum_in.at[*both, :], sum_send, sum_recv.at[2 if part == 1 else half], across)

    def own(t):
        return remote(own_out.at[t], own_in.at[t], sum_send, own_recv, partner)

    barrier = pltpu.get_barrier_semaphore()
    even = 1 - (p + c) % 2
    after, before = even * partner + (1 - even) * across, even * across + (1 - even) * partner
    pl.semaphore_signal(barrier, inc=1, device_id={"tp": after}, device_id_type=MESH)

    x_loads = [pltpu.make_async_copy(x.at[here, :], y.at[here, :], load_sem.at[n]) for n, here in enumerate(own_rows)]
    small = [pltpu.make_async_copy(a, b, load_sem.at[4 + n]) for n, (a, b) in enumerate(
        [(gain, gain_s), (table, table_s)])]
    w_loads = [pltpu.make_async_copy(a, b, w_sem.at[n // 3]) for n, (a, b) in enumerate([(wk, wk_s), (wv, wv_s), (wq, wq_s), (wo, wo_s)])]
    pl.semaphore_wait(barrier, 1)
    pl.semaphore_signal(met_sem, inc=1, device_id={"tp": before}, device_id_type=MESH)

    @pl.when(even == 1)
    def _():
        link(2 * c, 0).start()

    for load in (x_loads[0], small[0], *x_loads[1:]):
        load.start()

    def normed(t):
        wide = t.astype(f32)
        scale = lax.rsqrt(jnp.mean(wide * wide, -1, keepdims=True) + 1e-6)
        return (wide * scale * gain_s[...].reshape(1, WIDE).astype(f32)).astype(bf16)

    def norm(n):
        x_loads[n].wait()
        xn_s[pl.ds(pl.multiple_of(start + own_rows[n].start, ALIGN), own_rows[n].size), :] = normed(y[own_rows[n], :])

    @pl.when(even == 0)
    def _():
        pl.semaphore_wait(met_sem, 1)
        link(2 * c, 0).start()

    small[0].wait()
    norm(0)
    for load in small[1:] + w_loads:
        load.start()
    norm(1)

    @pl.when(c == 0)
    def _():
        link(0, 1).start()

    norm(2)

    @pl.when(even == 1)
    def _():
        pl.semaphore_wait(met_sem, 1)

    near(0).start()
    norm(3)

    @pl.when(c == 0)
    def _():
        link(1).start()

    near(1).start()

    near_in(0).wait_recv()

    @pl.when(c == 0)
    def _():
        link(2).start()

    @pl.when(c == 1)
    def _():
        link(0).start()

    near_in(1).wait_recv()

    @pl.when(c == 1)
    def _():
        link(1).start()
        link(2, 1).start()

    link(3).start()

    small[1].wait()
    pltpu.make_async_copy(xn_s, xn_s, w_sem.at[0]).wait()
    v_s[:, HEAD:, :] = jnp.ones((KV, 8, ROWS), bf16)
    gap_s[...] = lax.rem(lax.broadcasted_iota(jnp.int32, (PAIR, COLS), 1), PAIR) - lax.broadcasted_iota(jnp.int32, (PAIR, COLS), 0)

    def project(g, slot):
        cos, sin = table_s[pl.ds(2 * PAIR + g, 1), :], table_s[pl.ds(2 * PAIR + 8 + g, 1), :]
        first_cos, first_sin = table_s[:PAIR, :], table_s[PAIR : 2 * PAIR, :]
        cos_s[...] = first_cos * cos - first_sin * sin
        sin_s[...] = first_sin * cos + first_cos * sin
        at = pl.multiple_of(g * PAIR, PAIR)
        _project(xn_s.at[pl.ds(at, PAIR), :], wq_s, wk_s, wv_s, cos_s, sin_s, q_s.at[slot], k_s, v_s, at)

    def attend(slot, g):
        top_s[...] = jnp.full((KV, COLS), NEG, f32)
        mix_s[...] = jnp.zeros((KV, HEAD + 8, COLS), f32)

        def block(at, size, ok=None):
            _block(q_s.at[slot], k_s, v_s, top_s, mix_s, pl.multiple_of(at, PAIR), size, ok)

        lax.fori_loop(0, g // 2, lambda b, _: block(b * 2 * PAIR, 2 * PAIR), None)
        lax.fori_loop(0, g % 2, lambda b, _: block((g - 1) * PAIR, PAIR), None)
        block(g * PAIR, PAIR, gap_s[...] >= 0)
        _finish(mix_s, seen_s)

    def out(dst, at, n):
        for w in range(0, WIDE, 256):
            r = jnp.dot(seen_s[pl.ds(at, n), :], wo_s[:, w : w + 256], preferred_element_type=f32)
            dst[:, w : w + 256] = r.astype(dst.dtype)

    @pl.loop(0, 4)
    def _(t):
        i = (2 * c + t) % 4
        project(4 * p + i, i)

    link_in(0)
    forward(0).start()

    w_loads[3].wait()

    def send_total(j, parts=(2,)):
        term(j).wait_recv()
        sum_out[j] = (hold_s[j % 2] + term_in[j].astype(f32)).astype(bf16)
        for part in parts:
            total(j, part).start()

    @pl.loop(0, 4)
    def _(j):
        g = 4 * (1 - p) + j
        forward_in(j).wait_recv()
        project(g, 4)
        attend(4, g)

        @pl.when(j > 0)
        def _():
            send_total(j - 1)

        @pl.when(j < 3)
        def _():
            link_in(j + 1)
            forward(j + 1).start()

        out(term_out.at[j], pl.multiple_of(CHUNK * (1 - c), CHUNK), CHUNK)
        term(j).start()
        out(hold_s.at[j % 2], pl.multiple_of(CHUNK * c, CHUNK), CHUNK)

    send_total(3, (0, 1))

    @pl.loop(0, 4)
    def _(t):
        i = (2 * (1 - c) + t) % 4
        attend(i, 4 * p + i)
        out(own_s.at[t % 2], 0, PAIR)

        @pl.when(t < 2)
        def _():
            own_out[t] = own_s[t].astype(bf16)
            own(t).start()

    remote(own_out, own_in, sum_send, own_recv, partner).wait_recv()
    for t in range(2):
        own_s[t] = own_s[t] + y[t * PAIR : (t + 1) * PAIR, :].astype(f32) + own_in[t].astype(f32)

    def finished(half, part=2):
        total_in(half, part).wait_recv()
        at, n = piece[part].start, piece[part].size
        for i in range(2):
            y[pl.ds(PAIR * half + CHUNK * i + at, n), :] = (
                own_s[half, pl.ds(CHUNK * i + at, n), :] + sum_in[2 * half + i, pl.ds(at, n), :].astype(f32)).astype(bf16)

    finished(0)

    @pl.when(c == 0)
    def _():
        finished(1)

    @pl.when(c == 1)
    def _():
        finished(1, 0)
        finished(1, 1)

    remote(rows(0, 2048), rows(0, 2048), rows_send, near_recv.at[0], partner).wait_send()
    remote(rows(0, 1024), rows(0, 1024), sum_send, near_recv.at[0], partner).wait_send()


def _table():
    half = HEAD // 2
    rate = THETA ** (-np.arange(half, dtype=np.float64) / half)
    sign = np.repeat([-1.0, 1.0], half)

    def pair(places):
        angle = np.concatenate([places[:, None] * rate] * 2, axis=1)
        return np.cos(angle).astype(np.float32), (np.sin(angle) * sign).astype(np.float32)

    return np.concatenate([*pair(np.arange(PAIR, dtype=np.float64)), *pair(np.arange(0, ROWS, PAIR, dtype=np.float64))])


def solution(mesh):
    def step(x, gain, wq, wk, wv, wo):
        vmem, DMA, dma = pltpu.VMEM, pltpu.SemaphoreType.DMA, lambda n: pltpu.SemaphoreType.DMA((n,))
        return pl.pallas_call(
            _kernel,
            out_shape=pltpu.VMEM((512, WIDE), bf16),
            in_specs=[pl.BlockSpec(memory_space=pl.ANY)] * 7,
            out_specs=pl.BlockSpec(memory_space=pltpu.VMEM),
            scratch_shapes=[
                vmem((WIDE,), bf16), vmem((FIRST, WIDE), bf16),
                vmem((WIDE, 1024), bf16), vmem((WIDE, 512), bf16), vmem((WIDE, 512), bf16), vmem((1024, WIDE), bf16),
                vmem((2 * PAIR + 16, HEAD), f32),
                vmem((PAIR, HEAD), f32), vmem((PAIR, HEAD), f32),
                vmem((ROWS, WIDE), bf16), vmem((5, KV, COLS, HEAD), bf16), vmem((KV, ROWS, HEAD), bf16), vmem((KV, HEAD + 8, ROWS), bf16),
                vmem((KV, COLS), f32), vmem((KV, HEAD + 8, COLS), f32), vmem((PAIR, COLS), jnp.int32), vmem((PAIR, 1024), bf16),
                vmem((2, CHUNK, WIDE), f32),
                vmem((4, CHUNK, WIDE), bf16), vmem((4, CHUNK, WIDE), bf16), vmem((4, CHUNK, WIDE), bf16), vmem((4, CHUNK, WIDE), bf16),
                vmem((2, PAIR, WIDE), f32), vmem((2, PAIR, WIDE), bf16), vmem((2, PAIR, WIDE), bf16),
                dma(6), dma(2), DMA, DMA, dma(2), dma(5), dma(2), dma(2), dma(3), DMA, pltpu.SemaphoreType.REGULAR,
            ],
            compiler_params=pltpu.CompilerParams(collective_id=0, has_side_effects=True, vmem_limit_bytes=VMEM),
        )(x, gain, wq, wk, wv, wo, jnp.asarray(_table()))

    tokens, columns = P(("dp", "tp"), None), P(None, "tp")
    return jax.shard_map(
        step,
        mesh=mesh,
        in_specs=(tokens, P(None), columns, columns, columns, P("tp", None)),
        out_specs=tokens,
        check_vma=False,
    )
```
